128 devices in a mesh: dp: 16 (over x_lo, z, core), expert: 8 (over y, x_hi).
Axes of the slice: x: 4 (x_hi: 2, x_lo: 2; x = x_hi * 2 + x_lo), y: 4, z: 4, core: 2. Of those that a mesh axis runs over, the one named last changes fastest.
Arguments:
- tokens: bfloat16 [16384, 2048], P(('dp', 'expert')), may hold values from -6 to 6
- norm_gain: float32 [2048], replicated, may hold values from 0.25 to 1.75
- router_weight: bfloat16 [2048, 64], P('dp'), may hold values from -0.25 to 0.25
- expert_ids: int32 [16384, 8], P(('dp', 'expert')), may hold values from 0 to 63, all different within a row; in each aligned block of 128 rows (0 to 127, 128 to 255, ...) at most 32 rows name the same one
- gate_weight: bfloat16 [8, 2048, 1024], P('expert', 'dp'), may hold values from -0.125 to 0.125
- up_weight: bfloat16 [8, 2048, 1024], P('expert', 'dp'), may hold values from -0.125 to 0.125
- down_weight: bfloat16 [8, 2048, 1024], P('expert', 'dp'), may hold values from -0.1875 to 0.1875
- cotangent: bfloat16 [16384, 2048], P(('dp', 'expert')), may hold values from -6 to 6
Outputs:
- mixed: bfloat16 [16384, 2048], P(('dp', 'expert'))
- d_tokens: bfloat16 [16384, 2048], P(('dp', 'expert'))
- d_gain: float32 [2048], replicated
- d_router: float32 [2048, 64], P('dp')
- d_gate: bfloat16 [8, 2048, 1024], P('expert', 'dp')
- d_up: bfloat16 [8, 2048, 1024], P('expert', 'dp')
- d_down: bfloat16 [8, 2048, 1024], P('expert', 'dp')
The draws below stay inside these ranges and needn't reach their ends.
Inputs may be any that keep to these rules, and one draw needn't show every extreme that they name: `expert_ids`: each row names 8 different experts; in the rows of one device no expert is named more than 32 times.
All inputs are finite; a program needn't handle non-finite values.
Results may differ from the reference program's by a relative error of at most 0.018.
Values may be sent and summed in bfloat16 or wider, within the bound.
No kernel may reach another device: no remote copies, remote signals or barrier semaphores. Data moves between devices by JAX's collectives and lax.ppermute only.
A program may use at most 128 MiB of HBM per device.

```python
import math
import jax
import jax.numpy as jnp
import numpy as np
from jax import lax

D = 2048
FF = 1024
EXPERTS_ALL = 64
TOP = 8
TOK_DEV = 128
CAP = 32
EXPERTS = 8
TOKENS = 16384
N_DP = 16
N_EXPERT = 8


def steps_of(stream_key, extent, split, least, high):
    loudness, own = 1.0, jax.random.fold_in(stream_key, 6)
    for dim, blocks in split:
        draws = jnp.exp(jax.random.uniform(jax.random.fold_in(own, dim), (blocks,), jnp.float32, least / len(split), high / len(split)))
        loudness = loudness * jnp.repeat(draws, extent[dim] // blocks).reshape([-1 if axis == dim else 1 for axis in range(len(extent))])
    return loudness


def deal_out(stream_key, own, number, rows, amount, top, reach, skew):
    sequence = jax.random.permutation(stream_key, amount)
    heavy_load, ordinary = load_shares(amount, rows * top, reach, skew, True), load_shares(amount, rows * top, reach, skew, False)
    places = jnp.arange(amount)

    def named(sizes, rotation):
        used = int((sizes > 0).sum())
        fixed = max(1, used // 4)
        passed = fixed + (places - fixed + rotation * (used - fixed)) % max(1, amount - fixed)
        return jnp.zeros((amount,), jnp.int32).at[sequence[jnp.where(places < fixed, places, passed)]].set(jnp.asarray(sizes, jnp.int32))

    sizes = jnp.where(number % 4 == 0, named(heavy_load, number // 4), named(ordinary, number - number // 4 - 1))
    mixed = jax.random.permutation(jax.random.fold_in(own, 3), amount)
    source_of, taker = mixed[0:amount // 2 * 2:2], mixed[1:amount // 2 * 2:2]
    slack = jnp.minimum(sizes[source_of] - 1, reach - sizes[taker]) // 2
    slack = jnp.where((source_of == sequence[0]) | (taker == sequence[0]) | (sizes[taker] == 0), 0, jnp.maximum(slack, 0))
    passed = jax.random.randint(jax.random.fold_in(own, 4), (amount // 2,), 0, 1 << 20) % (slack + 1)
    sizes = sizes.at[source_of].add(-passed).at[taker].add(passed)
    labels = jnp.searchsorted(jnp.cumsum(sizes), jnp.arange(rows * top), side="right").astype(jnp.int32)
    grid = labels.reshape(top, rows).T
    grid = grid[jax.random.permutation(jax.random.fold_in(own, 1), rows)]
    rotation = jax.random.randint(jax.random.fold_in(own, 2), (rows, 1), 0, top)
    return jnp.take_along_axis(grid, (jnp.arange(top)[None, :] + rotation) % top, axis=1)


def load_shares(count, total, limit, lean, full):
    portions = [(1 << 20) // math.isqrt(standing ** lean) + 1 for standing in range(1, count + 1)]
    largest = limit if full else min(limit, max(-(-total // count), total * portions[0] // sum(portions)))
    least = 1 if total - largest >= count - 1 else 0
    holding, rest = [largest] + [least] * (count - 1), total - largest - least * (count - 1)
    while rest > 0:
        candidates = [i for i in range(1, count) if holding[i] < largest] or [i for i in range(1, count) if holding[i] < limit]
        mass, budget = sum([portions[i] for i in candidates]), rest
        for i in candidates:
            more = min(limit - holding[i], max(1, budget * portions[i] // mass), rest)
            holding[i] = holding[i] + more
            rest = rest - more
    return np.array(holding)


def gaussian(rng, extent, scale, limit, pieces=(), held_as=jnp.bfloat16):
    values = scale * jax.random.normal(rng, extent, jnp.float32)
    if pieces:
        values = values * steps_of(rng, extent, pieces, -0.22, 0.18)
    return jnp.clip(values, -limit, limit).astype(held_as)


def setup_inputs(seed: int = 0) -> dict:
    key_of = jax.random.split(jax.random.key(seed), 9)
    tokens = gaussian(key_of[0], (TOKENS, D), 1.0, 6.0, ((0, 128),))
    norm_gain = jnp.clip(1.0 + 0.15 * jax.random.normal(key_of[1], (D,), jnp.float32), 0.25, 1.75)
    router_weight = gaussian(key_of[2], (D, EXPERTS_ALL), (D // 4) ** -0.5, 0.25, ((0, 16),))
    expert_ids_keys = jax.random.split(jax.random.fold_in(key_of[3], 1), TOKENS // TOK_DEV)
    expert_ids_turns = jax.random.permutation(jax.random.fold_in(key_of[3], 3), TOKENS // TOK_DEV)
    expert_ids = jax.vmap(lambda own, number: deal_out(jax.random.fold_in(key_of[3], 2), own, number, TOK_DEV, EXPERTS_ALL, TOP, CAP, 1))(expert_ids_keys, expert_ids_turns).reshape((TOKENS, TOP))
    gate_weight = gaussian(key_of[4], (EXPERTS, D, FF), D ** -0.5, 0.125, ((0, 8), (1, 16)))
    up_weight = gaussian(key_of[5], (EXPERTS, D, FF), D ** -0.5, 0.125, ((0, 8), (1, 16)))
    down_weight = gaussian(key_of[6], (EXPERTS, D, FF), FF ** -0.5, 0.1875, ((0, 8), (1, 16)))
    cotangent = gaussian(key_of[7], (TOKENS, D), 1.0, 6.0, ((0, 128),))
    return {"tokens": tokens, "norm_gain": norm_gain, "router_weight": router_weight, "expert_ids": expert_ids, "gate_weight": gate_weight, "up_weight": up_weight, "down_weight": down_weight, "cotangent": cotangent}


EPSILON = 1e-05
HIGHEST = lax.Precision.HIGHEST

def normalize(inputs, norm_gain):
    meansq = lax.optimization_barrier(jnp.mean(inputs * inputs, axis=-1, keepdims=True))
    return inputs * lax.rsqrt(meansq + EPSILON) * norm_gain

def gate_weights(logits, expert_ids):
    member = (expert_ids[:, :, None] == jnp.arange(logits.shape[-1], dtype=jnp.int32)[None, None, :]).astype(jnp.float32)
    picked = lax.optimization_barrier(jnp.sum(member * logits[:, None, :], axis=-1))
    raised = jnp.exp(picked)
    return raised / lax.optimization_barrier(jnp.sum(raised, axis=-1, keepdims=True))

def pick_matrix(expert_ids, window, capacity):
    flat_ids = expert_ids.reshape(-1).astype(jnp.int32)
    chosen = (flat_ids[:, None] == jnp.arange(window, dtype=jnp.int32)[None, :]).astype(jnp.int32)
    before = (jnp.cumsum(chosen, axis=0, dtype=jnp.int32) - chosen).astype(jnp.int32)
    position = lax.optimization_barrier(jnp.sum(before * chosen, axis=-1)).astype(jnp.int32)
    target = jnp.where(flat_ids < window, flat_ids * capacity + position, -1).astype(jnp.int32)
    columns = jnp.arange(window * capacity, dtype=jnp.int32)
    matrix = (target[:, None] == columns[None, :]).astype(jnp.float32)
    return matrix.reshape(expert_ids.shape[0], expert_ids.shape[1], window * capacity)

def expert_forward(slot_rows, w_gate, w_up, w_down):
    gate_pre = jnp.dot(slot_rows, w_gate, preferred_element_type=jnp.float32)
    up_pre = jnp.dot(slot_rows, w_up, preferred_element_type=jnp.float32)
    active = (gate_pre * jax.nn.sigmoid(gate_pre) * up_pre).astype(jnp.bfloat16)
    output = jnp.dot(active, w_down.T, preferred_element_type=jnp.float32).astype(jnp.bfloat16)
    return (output, gate_pre, up_pre)

def expert_backward(slot_grads, gate_pre, up_pre, w_gate, w_up, w_down):
    sigmoid_gate = jax.nn.sigmoid(gate_pre)
    active = (gate_pre * sigmoid_gate * up_pre).astype(jnp.bfloat16)
    back = jnp.dot(slot_grads, w_down, preferred_element_type=jnp.float32)
    grad_gate = (back * up_pre * sigmoid_gate * (1.0 + gate_pre * (1.0 - sigmoid_gate))).astype(jnp.bfloat16)
    grad_upper = (back * gate_pre * sigmoid_gate).astype(jnp.bfloat16)
    grad_rows = jnp.dot(grad_gate, w_gate.T, preferred_element_type=jnp.float32)
    grad_rows = (grad_rows + jnp.dot(grad_upper, w_up.T, preferred_element_type=jnp.float32)).astype(jnp.bfloat16)
    return (grad_rows, active, grad_gate, grad_upper)

def group_terms(slot_rows, slot_grads, active, grad_gate, grad_upper):
    rows_wide = slot_rows.astype(jnp.float32)
    term_gate = jnp.einsum('krd,krf->kdf', rows_wide, grad_gate.astype(jnp.float32), precision=HIGHEST)
    term_upper = jnp.einsum('krd,krf->kdf', rows_wide, grad_upper.astype(jnp.float32), precision=HIGHEST)
    term_down = jnp.einsum('krd,krf->kdf', slot_grads.astype(jnp.float32), active.astype(jnp.float32), precision=HIGHEST)
    stacked = jnp.concatenate([term_gate, term_upper, term_down], axis=-1)
    rounded = lax.optimization_barrier(stacked.astype(jnp.bfloat16)).astype(jnp.float32)
    return lax.optimization_barrier(jnp.sum(rounded, axis=0))

def reference(tokens, norm_gain, router_weight, expert_ids, gate_weight, up_weight, down_weight, cotangent):
    blocks = N_DP * N_EXPERT
    slot_count = EXPERTS * CAP
    inputs = tokens.astype(jnp.float32)
    hidden = normalize(inputs, norm_gain).astype(jnp.bfloat16)
    logits = jnp.dot(hidden, router_weight, preferred_element_type=jnp.float32)
    weights, gate_back = jax.vjp(lambda values: gate_weights(values, expert_ids), logits)
    pick_table = jax.vmap(lambda block_ids: pick_matrix(block_ids, EXPERTS, CAP))(expert_ids.reshape(blocks, TOK_DEV, TOP))
    spread = lax.optimization_barrier(jnp.sum(pick_table, axis=2))
    blending = jnp.einsum('btks,btk->bts', pick_table, weights.reshape(blocks, TOK_DEV, TOP), precision=HIGHEST)
    hidden_blocks = hidden.reshape(blocks, TOK_DEV, D).astype(jnp.float32)
    cot_blocks = cotangent.reshape(blocks, TOK_DEV, D).astype(jnp.float32)
    outgoing = jnp.einsum('bts,btd->bsd', spread, hidden_blocks, precision=HIGHEST).astype(jnp.bfloat16)
    outgoing_grad = jnp.einsum('bts,btd->bsd', blending, cot_blocks, precision=HIGHEST).astype(jnp.bfloat16)

    def arrange(values):
        shaped = values.reshape(N_DP, N_EXPERT, EXPERTS, CAP, D).transpose(2, 0, 1, 3, 4)
        return shaped.reshape(EXPERTS, N_DP, N_EXPERT * CAP, D)

    def restore(values):
        shaped = values.reshape(EXPERTS, N_DP, N_EXPERT, CAP, D).transpose(1, 2, 0, 3, 4)
        return shaped.reshape(blocks, slot_count, D)

    def one_expert(operands):
        slot_rows, slot_grads, w_gate, w_up, w_down = operands
        flat_rows = slot_rows.reshape(-1, D)
        flat_grads = slot_grads.reshape(-1, D)
        output, gate_pre, up_pre = expert_forward(flat_rows, w_gate, w_up, w_down)
        grad_rows, active, grad_gate, grad_upper = expert_backward(flat_grads, gate_pre, up_pre, w_gate, w_up, w_down)
        summed = group_terms(slot_rows, slot_grads, active.reshape(N_DP, -1, FF), grad_gate.reshape(N_DP, -1, FF), grad_upper.reshape(N_DP, -1, FF))
        return (output.reshape(slot_rows.shape), grad_rows.reshape(slot_rows.shape), summed)
    outputs, grad_slots, weight_grads = lax.map(one_expert, (arrange(outgoing), arrange(outgoing_grad), gate_weight, up_weight, down_weight))
    returned = restore(outputs).astype(jnp.float32)
    returned_grad = restore(grad_slots).astype(jnp.float32)
    mixed_out = jnp.einsum('bts,bsd->btd', blending, returned, precision=HIGHEST).astype(jnp.bfloat16).reshape(-1, D)
    gathered_cot = jnp.einsum('bts,btd->bsd', spread, cot_blocks, precision=HIGHEST)
    per_slot = lax.optimization_barrier(jnp.sum(gathered_cot * returned, axis=-1))
    grad_weights = jnp.einsum('btks,bs->btk', pick_table, per_slot, precision=HIGHEST).reshape(-1, TOP)
    grad_logits = gate_back(grad_weights)[0]
    grad_hidden = jnp.einsum('bts,bsd->btd', spread, returned_grad, precision=HIGHEST).reshape(-1, D)
    grad_hidden = grad_hidden + jnp.dot(grad_logits, router_weight.astype(jnp.float32).T, precision=HIGHEST)
    unused_value, norm_back = jax.vjp(normalize, inputs, norm_gain)
    grad_inputs, grad_gain = norm_back(grad_hidden)
    grad_router = jnp.dot(hidden.astype(jnp.float32).T, grad_logits, precision=HIGHEST)
    grad_gate_out = weight_grads[:, :, :FF].astype(jnp.bfloat16)
    grad_up_out = weight_grads[:, :, FF:2 * FF].astype(jnp.bfloat16)
    grad_down_out = weight_grads[:, :, 2 * FF:].astype(jnp.bfloat16)
    return (mixed_out, grad_inputs.astype(jnp.bfloat16), grad_gain, grad_router, grad_gate_out, grad_up_out, grad_down_out)
```

```python
import jax
import jax.numpy as jnp
from jax import lax
from jax.experimental import pallas as pl
from jax.experimental.pallas import tpu as pltpu
from jax.sharding import PartitionSpec as P

D = 2048
FF = 1024
CAP = 32
TOK = 128
WIN = 8
SLOTS = WIN * CAP
EPSILON = 1e-05
BK = 256
FC = 256
CHIPS = 8
F32 = jnp.float32
BF = jnp.bfloat16


def nn(a, b):
    return lax.dot_general(a, b, (((1,), (0,)), ((), ())), preferred_element_type=F32)


def nt(a, b):
    return lax.dot_general(a, b, (((1,), (1,)), ((), ())), preferred_element_type=F32)


def tn(a, b):
    return lax.dot_general(a, b, (((0,), (0,)), ((), ())), preferred_element_type=F32)


def split(v):
    high = v.astype(BF)
    return high, (v - high.astype(F32)).astype(BF)


def sds(shape, dtype):
    return jax.ShapeDtypeStruct(shape, dtype)


SMEM = pl.BlockSpec(memory_space=pltpu.SMEM)
VMEM = pl.BlockSpec(memory_space=pltpu.VMEM)


def call(kernel, name, out_shape, *args, smem=0):
    outs = out_shape if isinstance(out_shape, (list, tuple)) else [out_shape]
    specs = [SMEM] * smem + [VMEM] * (len(args) - smem)
    return pl.pallas_call(
        kernel,
        name=name,
        out_shape=out_shape,
        in_specs=specs,
        out_specs=[VMEM] * len(outs) if isinstance(out_shape, (list, tuple)) else VMEM,
    )(*args)


def at(ref_index, block=BK):
    return pl.ds(pl.multiple_of(ref_index, block), block)


def pack_kernel(place, gate, up, down, router_t, away, keep):
    core = place[8]
    for k in range(2):
        for m, w in enumerate((gate, up, down)):
            rows = pl.ds((k * 3 + m) * TOK, TOK)
            keep[rows, :] = w[:, at(core * 512 + k * FC)]
            away[rows, :] = w[:, at((1 - core) * 512 + k * FC)]
    away[pl.ds(768, 32), pl.ds(0, 128)] = router_t[pl.ds(0, 32), :]
    away[pl.ds(768, 32), pl.ds(128, 128)] = router_t[pl.ds(32, 32), :]


def join_kernel(place, mine, router_t, other, first, second):
    core = place[8]
    for k, out in enumerate((first, second)):
        for m in range(3):
            rows = pl.ds((k * 3 + m) * TOK, TOK)
            out[at(m * BK + core * TOK, TOK), :] = mine[rows, :]
            out[at(m * BK + (1 - core) * TOK, TOK), :] = other[rows, :]
    first[pl.ds(768, 64), at(core * TOK, TOK)] = router_t[...]
    first[pl.ds(768, 32), at((1 - core) * TOK, TOK)] = other[pl.ds(768, 32), pl.ds(0, 128)]
    first[pl.ds(800, 32), at((1 - core) * TOK, TOK)] = other[pl.ds(768, 32), pl.ds(128, 128)]


def dispatch_kernel(place, tokens, cotangent, gain, ids, hidden, xs, gains, root, spread, chosen, outgoing):
    lane = lax.broadcasted_iota(jnp.int32, (TOK, 128), 1)
    picked = jnp.zeros((TOK, 128), F32)
    for k in range(8):
        picked = picked + (ids[:, k : k + 1] == lane).astype(F32)
    chosen[...] = picked
    half = picked.astype(BF)
    row = lax.broadcasted_iota(jnp.int32, (TOK, TOK), 0)
    col = lax.broadcasted_iota(jnp.int32, (TOK, TOK), 1)
    earlier = nn((col < row).astype(F32).astype(BF), half)
    who = lax.broadcasted_iota(jnp.int32, (128, SLOTS), 0)
    slot = lax.broadcasted_iota(jnp.int32, (128, SLOTS), 1)
    widen = (who == slot // CAP).astype(F32).astype(BF)
    position = nn(earlier.astype(BF), widen)
    named = nn(half, widen)
    column = lax.broadcasted_iota(jnp.int32, (TOK, SLOTS), 1)
    table = jnp.where(
        (named > 0.5) & (position == (column % CAP).astype(F32)), 1.0, 0.0
    ).astype(BF)
    spread[...] = table
    total = jnp.zeros((TOK, 1), F32)
    for b in range(CHIPS):
        x = tokens[:, at(place[b] * BK)]
        xs[:, b * BK : (b + 1) * BK] = x
        x = x.astype(F32)
        total = total + jnp.sum(x * x, axis=-1, keepdims=True)
    r = lax.rsqrt(total * (1.0 / D) + EPSILON)
    root[...] = jnp.broadcast_to(r, (TOK, 128))
    for b in range(CHIPS):
        cols = slice(b * BK, (b + 1) * BK)
        g = gain[:, at(place[b] * BK)]
        gains[:, cols] = g
        h = (xs[:, cols].astype(F32) * r * g).astype(BF)
        hidden[:, cols] = h
        outgoing[:, cols] = tn(table, h).astype(BF)
        outgoing[:, D + b * BK : D + (b + 1) * BK] = tn(
            table, cotangent[:, at(place[b] * BK)]
        ).astype(BF)


def router_kernel(*refs):
    hidden, spread, chosen = refs[:3]
    pieces = refs[3:11]
    routed, weight, blend_high, blend_low, slot_weight = refs[11:]
    logits = jnp.zeros((TOK, 64), F32)
    for b, piece in enumerate(pieces):
        r = piece[768:832, :]
        routed[:, b * BK : (b + 1) * BK] = r
        logits = logits + nt(hidden[:, b * BK : (b + 1) * BK], r)
    picked = chosen[:, :64] > 0.5
    raised = jnp.where(picked, jnp.exp(logits), 0.0)
    w = raised / jnp.sum(raised, axis=-1, keepdims=True)
    weight[...] = w
    who = lax.broadcasted_iota(jnp.int32, (64, SLOTS), 0)
    slot = lax.broadcasted_iota(jnp.int32, (64, SLOTS), 1)
    widen = (who == slot // CAP).astype(F32).astype(BF)
    high, low = split(w)
    table = spread[...]
    bh = (nn(high, widen) * table.astype(F32)).astype(BF)
    bl = (nn(low, widen) * table.astype(F32)).astype(BF)
    blend_high[...] = bh
    blend_low[...] = bl
    ones = jnp.ones((TOK, 128), BF)
    slot_weight[...] = tn(bh, ones) + tn(bl, ones)


def flip_kernel(mine, other, flipped):
    for b in range(16):
        cols = slice(b * BK, (b + 1) * BK)
        flipped[cols, 0:SLOTS] = mine[:, cols].T
        flipped[cols, SLOTS : 2 * SLOTS] = other[:, cols].T


def hidden_kernel(*refs):
    rows = refs[:2]
    weights = refs[2:4]
    pieces = refs[4:12]
    act, scaled, grad_gate, grad_up = refs[12:]
    for i in range(2):
        gate = jnp.zeros((SLOTS, FC), F32)
        up = jnp.zeros((SLOTS, FC), F32)
        back = jnp.zeros((SLOTS, FC), F32)
        for b, piece in enumerate(pieces):
            x = rows[i][:, b * BK : (b + 1) * BK]
            gate = gate + nn(x, piece[0:256, :])
            up = up + nn(x, piece[256:512, :])
            back = back + nn(rows[i][:, D + b * BK : D + (b + 1) * BK], piece[512:768, :])
        out = slice(i * SLOTS, (i + 1) * SLOTS)
        w = weights[i][:, 0:1]
        sig = jax.nn.sigmoid(gate)
        silu = gate * sig
        active = silu * up
        back = back * w
        act[out, :] = active.astype(BF)
        scaled[out, :] = (active * w).astype(BF)
        grad_gate[out, :] = (back * up * sig * (1.0 + gate * (1.0 - sig))).astype(BF)
        grad_up[out, :] = (back * silu).astype(BF)


def output_kernel(*refs):
    acts = refs[:2]
    pieces = (refs[2:10], refs[10:18])
    outs = refs[18:]
    for i in range(2):
        rows = slice(i * SLOTS, (i + 1) * SLOTS)
        for b in range(CHIPS):
            total = nt(acts[0][rows, :], pieces[0][b][512:768, :])
            total = total + nt(acts[1][rows, :], pieces[1][b][512:768, :])
            outs[i][:, b * BK : (b + 1) * BK] = total.astype(BF)


def back_kernel(*refs):
    gates = refs[:2]
    ups = refs[2:4]
    pieces = (refs[4:12], refs[12:20])
    outs = refs[20:]
    for i in range(2):
        rows = slice(i * SLOTS, (i + 1) * SLOTS)
        for b in range(CHIPS):
            total = nt(gates[0][rows, :], pieces[0][b][0:256, :])
            total = total + nt(ups[0][rows, :], pieces[0][b][256:512, :])
            total = total + nt(gates[1][rows, :], pieces[1][b][0:256, :])
            total = total + nt(ups[1][rows, :], pieces[1][b][256:512, :])
            outs[i][:, b * BK : (b + 1) * BK] = total.astype(BF)


def grads_kernel(flipped, scaled, grad_gate, grad_up, *outs):
    for b in range(CHIPS):
        x = flipped[b * BK : (b + 1) * BK, :]
        outs[b][0:256, :] = nn(x, grad_gate[...]).astype(BF)
        outs[b][256:512, :] = nn(x, grad_up[...]).astype(BF)
        outs[b][512:768, :] = nn(flipped[D + b * BK : D + (b + 1) * BK, :], scaled[...]).astype(BF)


def mix_kernel(place, returned, sent, blend_high, blend_low, spread, weight, hidden, mixed, grad_logits, router_part):
    per_slot = jnp.zeros((SLOTS, 1), F32)
    for b in range(CHIPS):
        cols = slice(b * BK, (b + 1) * BK)
        y = returned[:, cols]
        mixed[:, at(place[b] * BK)] = (nn(blend_high[...], y) + nn(blend_low[...], y)).astype(BF)
        per_slot = per_slot + jnp.sum(
            sent[:, D + b * BK : D + (b + 1) * BK].astype(F32) * y.astype(F32),
            axis=-1,
            keepdims=True,
        )
    slot = lax.broadcasted_iota(jnp.int32, (SLOTS, 64), 0)
    who = lax.broadcasted_iota(jnp.int32, (SLOTS, 64), 1)
    spots = jnp.where(who == slot // CAP, per_slot, 0.0)
    high = spots.astype(BF)
    rest = spots - high.astype(F32)
    middle = rest.astype(BF)
    low = (rest - middle.astype(F32)).astype(BF)
    table = spread[...]
    grad_weights = nn(table, high) + nn(table, middle) + nn(table, low)
    w = weight[...]
    inner = jnp.sum(w * grad_weights, axis=-1, keepdims=True)
    g = w * (grad_weights - inner)
    grad_logits[...] = g
    gh, gl = split(g)
    for b in range(CHIPS):
        h = hidden[:, b * BK : (b + 1) * BK]
        part = (tn(gh, h) + tn(gl, h)).astype(BF)
        for c in range(2):
            router_part[place[b] * 2 + c] = part[:, c * TOK : (c + 1) * TOK]


def norm_kernel(place, returned, spread, grad_logits, routed, xs, gains, root, d_tokens, gain_part, work):
    gh, gl = split(grad_logits[...])
    r = root[:, 0:1]
    inner = jnp.zeros((TOK, 1), F32)
    for b in range(CHIPS):
        cols = slice(b * BK, (b + 1) * BK)
        rt = routed[:, cols]
        grad = nn(spread[...], returned[:, cols]) + nn(gh, rt) + nn(gl, rt)
        x = xs[:, cols].astype(F32)
        gain_part[pl.ds(place[b], 1), :] = jnp.sum(grad * x * r, axis=0, keepdims=True)
        scaled = grad * gains[:, cols]
        work[:, cols] = scaled
        inner = inner + jnp.sum(scaled * x, axis=-1, keepdims=True)
    factor = inner * (r * r * r) * (1.0 / D)
    for b in range(CHIPS):
        cols = slice(b * BK, (b + 1) * BK)
        d_tokens[:, at(place[b] * BK)] = (
            work[:, cols] * r - xs[:, cols].astype(F32) * factor
        ).astype(BF)


def perm(move):
    pairs = []
    for x in range(2):
        for z in range(4):
            for c in range(2):
                tx, tz, tc = move(x, z, c)
                pairs.append(((x * 4 + z) * 2 + c, (tx * 4 + tz % 4) * 2 + tc))
    return pairs


SIBLING = perm(lambda x, z, c: (x, z, 1 - c))
ACROSS = perm(lambda x, z, c: (1 - x, z, c))
AHEAD = perm(lambda x, z, c: (x, z + 1, c))
BEHIND = perm(lambda x, z, c: (x, z + 3, c))


def send(v, pairs):
    return lax.ppermute(v, "dp", pairs)


def gather_pieces(own):
    across = send(own, ACROSS)
    own_3 = send(own, AHEAD)
    own_1 = send(own, BEHIND)
    across_3 = send(across, AHEAD)
    across_1 = send(across, BEHIND)
    own_2 = send(own_3, AHEAD)
    across_2 = send(across_1, BEHIND)
    return (own, own_1, own_2, own_3, across, across_1, across_2, across_3)


def plus(*values):
    total = values[0].astype(F32)
    for v in values[1:]:
        total = total + v.astype(F32)
    return total.astype(BF)


def reduce_pieces(parts):
    own_2 = send(parts[2], AHEAD)
    across_2 = send(parts[6], BEHIND)
    across_1 = send(parts[5], AHEAD)
    own_3 = send(parts[3], BEHIND)
    own_1 = send(plus(parts[1], own_2), AHEAD)
    across_3 = send(plus(parts[7], across_2), BEHIND)
    across = send(plus(parts[4], across_1, across_3), ACROSS)
    return plus(parts[0], own_1, own_3, across)


def exchange(v, axis):
    return lax.all_to_all(v, axis, split_axis=0, concat_axis=0, tiled=True)


def body(
    tokens, norm_gain, router_weight, expert_ids, gate_weight, up_weight, down_weight, cotangent
):
    spot = lax.axis_index("dp")
    core = spot % 2
    chip = spot // 2
    x, z = chip // 4, chip % 4
    rel = jnp.arange(8, dtype=jnp.int32)
    order = ((x ^ (rel // 4)) * 4 + (z + rel % 4) % 4).astype(jnp.int32)
    place = jnp.concatenate([order, core[None].astype(jnp.int32)])

    router_t = router_weight.T
    away, keep = call(
        pack_kernel, "pack", [sds((800, FC), BF), sds((768, FC), BF)],
        place, gate_weight[0], up_weight[0], down_weight[0], router_t, smem=1,
    )
    other = send(away, SIBLING)
    first, second = call(
        join_kernel, "join", [sds((832, FC), BF), sds((768, FC), BF)],
        place, keep, router_t, other, smem=1,
    )
    pieces = (gather_pieces(first), gather_pieces(second))

    hidden, xs, gains, root, spread, chosen, sent = call(
        dispatch_kernel, "dispatch",
        [sds((TOK, D), BF), sds((TOK, D), BF), sds((1, D), F32), sds((TOK, 128), F32),
         sds((TOK, SLOTS), BF), sds((TOK, 128), F32), sds((SLOTS, 2 * D), BF)],
        place, tokens, cotangent, norm_gain[None], expert_ids, smem=1,
    )
    rows = exchange(sent.reshape(WIN, CAP, 2 * D), "expert").reshape(SLOTS, 2 * D)
    rows_other = send(rows, SIBLING)
    flipped = call(flip_kernel, "flip", sds((2 * D, 2 * SLOTS), BF), rows, rows_other)

    routed, weight, blend_high, blend_low, slot_weight = call(
        router_kernel, "router",
        [sds((64, D), BF), sds((TOK, 64), F32), sds((TOK, SLOTS), BF), sds((TOK, SLOTS), BF),
         sds((SLOTS, 128), F32)],
        hidden, spread, chosen, *pieces[0],
    )
    w_rows = exchange(slot_weight.reshape(WIN, CAP, 128), "expert").reshape(SLOTS, 128)
    w_other = send(w_rows, SIBLING)

    halves = []
    for k in range(2):
        halves.append(call(
            hidden_kernel, f"hidden{k}", [sds((2 * SLOTS, FC), BF)] * 4,
            rows, rows_other, w_rows, w_other, *pieces[k],
        ))
    partial, partial_other = call(
        output_kernel, "output", [sds((SLOTS, D), BF)] * 2,
        halves[0][0], halves[1][0], *pieces[0], *pieces[1],
    )
    output = plus(partial, send(partial_other, SIBLING))
    returned = exchange(output.reshape(WIN, CAP, D), "expert").reshape(SLOTS, D)
    back, back_other = call(
        back_kernel, "back", [sds((SLOTS, D), BF)] * 2,
        halves[0][2], halves[1][2], halves[0][3], halves[1][3], *pieces[0], *pieces[1],
    )
    slot_back = plus(back, send(back_other, SIBLING))
    returned_back = exchange(slot_back.reshape(WIN, CAP, D), "expert").reshape(SLOTS, D)

    sums = []
    for k in range(2):
        _, scaled, grad_gate, grad_up = halves[k]
        parts = call(
            grads_kernel, f"grads{k}", [sds((768, FC), BF)] * 8,
            flipped, scaled, grad_gate, grad_up,
        )
        sums.append(reduce_pieces(parts).reshape(3, 2, TOK, FC))
    both = jnp.stack(sums)
    mine = lax.dynamic_index_in_dim(both, core, axis=2, keepdims=False)
    theirs = send(lax.dynamic_index_in_dim(both, 1 - core, axis=2, keepdims=False), SIBLING)
    low = jnp.where(core == 0, mine, theirs)
    high = jnp.where(core == 0, theirs, mine)
    d_weights = [
        jnp.concatenate([low[0, m], low[1, m], high[0, m], high[1, m]], axis=1)[None]
        for m in range(3)
    ]

    mixed, grad_logits, router_part = call(
        mix_kernel, "mix",
        [sds((TOK, D), BF), sds((TOK, 64), F32), sds((16, 64, TOK), BF)],
        place, returned, sent, blend_high, blend_low, spread, weight, hidden, smem=1,
    )
    router_sum = jnp.sum(exchange(router_part, "dp").astype(F32), axis=0)

    d_tokens, gain_part = pl.pallas_call(
        norm_kernel,
        name="norm",
        out_shape=[sds((TOK, D), BF), sds((CHIPS, BK), F32)],
        in_specs=[SMEM] + [VMEM] * 7,
        out_specs=[VMEM, VMEM],
        scratch_shapes=[pltpu.VMEM((TOK, D), F32)],
    )(place, returned_back, spread, grad_logits, routed, xs, gains, root)

    small = jnp.concatenate([router_sum, gain_part.reshape(16, 128)], axis=0)
    small = exchange(jnp.broadcast_to(small, (8, 80, 128)), "expert")
    small = jnp.sum(small, axis=0)
    d_router = small[:64].T
    gain = exchange(jnp.broadcast_to(small[64:], (16, 16, 128)), "dp")
    d_gain = jnp.sum(gain, axis=0).reshape(D)
    return (mixed, d_tokens, d_gain, d_router, *d_weights)


def solution(mesh):
    in_specs = (
        P(("dp", "expert"), None),
        P(),
        P("dp", None),
        P(("dp", "expert"), None),
        P("expert", "dp", None),
        P("expert", "dp", None),
        P("expert", "dp", None),
        P(("dp", "expert"), None),
    )
    out_specs = (
        P(("dp", "expert"), None),
        P(("dp", "expert"), None),
        P(),
        P("dp", None),
        P("expert", "dp", None),
        P("expert", "dp", None),
        P("expert", "dp", None),
    )
    return jax.shard_map(body, mesh=mesh, in_specs=in_specs, out_specs=out_specs, check_vma=False)
```

```python
import jax
import jax.numpy as jnp
from jax import lax
from jax.experimental import pallas as pl
from jax.experimental.pallas import tpu as pltpu
from jax.sharding import Mesh
from jax.sharding import PartitionSpec as P


D = 2048
FF = 1024
CAP = 32
TOK = 128
WIN = 8
SLOTS = WIN * CAP
EPSILON = 1e-05
BK = 256
HALF = 512
WIDE = 2 * D + 128
ROWS = 800
CHIPS = 8
F32 = jnp.float32
BF = jnp.bfloat16


def nn(a, b):
    return lax.dot_general(a, b, (((1,), (0,)), ((), ())), preferred_element_type=F32)


def nt(a, b):
    return lax.dot_general(a, b, (((1,), (1,)), ((), ())), preferred_element_type=F32)


def tn(a, b):
    return lax.dot_general(a, b, (((0,), (0,)), ((), ())), preferred_element_type=F32)


def split(v):
    high = v.astype(BF)
    return high, (v - high.astype(F32)).astype(BF)


def sds(shape, dtype):
    return jax.ShapeDtypeStruct(shape, dtype)


SMEM = pl.BlockSpec(memory_space=pltpu.SMEM)
VMEM = pl.BlockSpec(memory_space=pltpu.VMEM)
HBM = pl.BlockSpec(memory_space=pltpu.HBM)


def call(kernel, out_shape, *args, smem=0, near=True, limit=None, scratch=(), far=(), dram=(), far_out=False):
    outs = out_shape if isinstance(out_shape, (list, tuple)) else [out_shape]
    specs = [SMEM] * smem + [VMEM] * (len(args) - smem)
    for i in far:
        specs[i] = HBM
    out_spec = HBM if far_out else VMEM
    if near:
        args = args[:smem] + tuple(
            pltpu.with_memory_space_constraint(v, pltpu.HBM) if i + smem in far or i + smem in dram else pltpu.with_memory_space_constraint(v, pltpu.VMEM)
            for i, v in enumerate(args[smem:])
        )
    params = pltpu.CompilerParams(vmem_limit_bytes=limit) if limit else None
    return pl.pallas_call(
        kernel,
        out_shape=out_shape,
        in_specs=specs,
        out_specs=[out_spec] * len(outs) if isinstance(out_shape, (list, tuple)) else out_spec,
        scratch_shapes=list(scratch),
        compiler_params=params,
    )(*args)


def at(ref_index, block=BK):
    return pl.ds(pl.multiple_of(ref_index, block), block)


def pack_kernel(place, gate, up, down, router_t, away, keep, sems):
    copies = []
    for m, w in enumerate((gate, up, down)):
        for j, (out, side) in enumerate(((away, 1 - place[8]), (keep, place[8]))):
            copies.append(
                pltpu.make_async_copy(
                    w.at[:, at(side * HALF, HALF)], out.at[m * TOK : (m + 1) * TOK, :], sems.at[j, m]
                )
            )
    for c in copies:
        c.start()
    for g in range(4):
        for out in (away, keep):
            out[384:400, g * TOK : (g + 1) * TOK] = router_t[g * 16 : (g + 1) * 16, :]
    for c in copies:
        c.wait()


def join_kernel(place, keep, other, own):
    core = place[8]
    for source, side in ((keep, core), (other, 1 - core)):
        for m in range(3):
            own[at(m * BK + side * TOK, TOK), :] = source[m * TOK : (m + 1) * TOK, :]
        own[at(768 + side * 16, 16), :] = source[384:400, :]


def router_rows(piece, c):
    rows = piece[768 + c * 16 : 784 + c * 16, :]
    return jnp.concatenate([rows[:, g * TOK : (g + 1) * TOK] for g in range(4)], axis=0)


def dispatch_kernel(place, tokens, cotangent, gain, ids, hidden, xs, gains, root, spread, chosen, outgoing):
    lane = lax.broadcasted_iota(jnp.int32, (TOK, 128), 1)
    picked = jnp.zeros((TOK, 128), F32)
    for k in range(8):
        picked = picked + (ids[:, k : k + 1] == lane).astype(F32)
    chosen[...] = picked
    half = picked.astype(BF)
    row = lax.broadcasted_iota(jnp.int32, (TOK, TOK), 0)
    col = lax.broadcasted_iota(jnp.int32, (TOK, TOK), 1)
    earlier = nn((col < row).astype(F32).astype(BF), half)
    who = lax.broadcasted_iota(jnp.int32, (128, SLOTS), 0)
    slot = lax.broadcasted_iota(jnp.int32, (128, SLOTS), 1)
    widen = (who == slot // CAP).astype(F32).astype(BF)
    position = nn(earlier.astype(BF), widen)
    named = nn(half, widen)
    column = lax.broadcasted_iota(jnp.int32, (TOK, SLOTS), 1)
    table = jnp.where(
        (named > 0.5) & (position == (column % CAP).astype(F32)), 1.0, 0.0
    ).astype(BF)
    spread[...] = table
    total = jnp.zeros((TOK, 1), F32)
    for b in range(CHIPS):
        x = tokens[:, at(place[b] * BK)]
        xs[:, b * BK : (b + 1) * BK] = x
        x = x.astype(F32)
        total = total + jnp.sum(x * x, axis=-1, keepdims=True)
    r = lax.rsqrt(total * (1.0 / D) + EPSILON)
    root[...] = jnp.broadcast_to(r, (TOK, 128))
    for b in range(CHIPS):
        cols = slice(b * BK, (b + 1) * BK)
        g = gain[:, at(place[b] * BK)]
        gains[:, cols] = g
        h = (xs[:, cols].astype(F32) * r * g).astype(BF)
        hidden[:, cols] = h
        outgoing[:, cols] = tn(table, h).astype(BF)
        outgoing[:, D + b * BK : D + (b + 1) * BK] = tn(
            table, cotangent[:, at(place[b] * BK)]
        ).astype(BF)
    outgoing[:, 2 * D :] = tn(table, half).astype(BF)


def flip_kernel(mine, other, flipped):
    for b in range(16):
        cols = slice(b * BK, (b + 1) * BK)
        flipped[cols, 0:SLOTS] = mine[:, cols].T
        flipped[cols, SLOTS : 2 * SLOTS] = other[:, cols].T


EARLY = (0, 1, 3, 4, 2, 5)
LATE = (7, 6)


def products(rows, pieces, blocks, totals, logits):
    for b, piece in zip(blocks, pieces):
        x = rows[:, b * BK : (b + 1) * BK]
        y = rows[:, D + b * BK : D + (b + 1) * BK]
        totals[0] = totals[0] + nn(x, piece[0:256, :])
        totals[1] = totals[1] + nn(x, piece[256:512, :])
        totals[2] = totals[2] + nn(y, piece[512:768, :])
        for c in range(2):
            logits = logits + nt(x[:, c * TOK : (c + 1) * TOK], router_rows(piece, c))
    return totals, logits


def fetch(sources, held, sems):
    copies = [
        pltpu.make_async_copy(source, held.at[n], sems.at[n]) for n, source in enumerate(sources)
    ]
    for c in copies:
        c.start()
    for c in copies:
        c.wait()
    return [held.at[n] for n in range(len(copies))]


def keep_products(rows, pieces, sums, slot_logits):
    totals, logits = products(
        rows, pieces, EARLY, [jnp.zeros((SLOTS, HALF), F32)] * 3, jnp.zeros((SLOTS, 64), F32)
    )
    for m in range(3):
        sums[:, m * HALF : (m + 1) * HALF] = totals[m]
    slot_logits[...] = logits


def early_kernel(rows, *refs):
    sums, slot_logits, routed, held, sems = refs[6:]
    pieces = fetch(refs[:6], held, sems)
    keep_products(rows, pieces, sums, slot_logits)
    for n in range(6):
        for c in range(2):
            routed[:, (2 * n + c) * TOK : (2 * n + c + 1) * TOK] = router_rows(pieces[n], c)


def early_other_kernel(rows, held, sums, slot_logits):
    keep_products(rows, [held.at[n] for n in range(6)], sums, slot_logits)


def late_kernel(place, *refs):
    act, scaled, grad_gate, grad_up, routed, held, sems = refs[8:]
    pieces = fetch(refs[6:8], held, sems)
    lane = lax.broadcasted_iota(jnp.int32, (SLOTS, 64), 1)
    for i in range(2):
        rows, sums, slot_logits = refs[3 * i : 3 * i + 3]
        out = slice(i * SLOTS, (i + 1) * SLOTS)
        totals, logits = products(
            rows, pieces, LATE, [sums[:, m * HALF : (m + 1) * HALF] for m in range(3)],
            slot_logits[...],
        )
        picked = rows[:, 2 * D : 2 * D + 64].astype(F32) > 0.5
        raised = jnp.where(picked, jnp.exp(logits), 0.0)
        mine = jnp.sum(jnp.where(lane == place[9], raised, 0.0), axis=-1, keepdims=True)
        total = jnp.sum(raised, axis=-1, keepdims=True)
        w = jnp.where(total > 0.0, mine / jnp.where(total > 0.0, total, 1.0), 0.0)
        gate, up, back = totals
        sig = jax.nn.sigmoid(gate)
        silu = gate * sig
        active = silu * up
        back = back * w
        act[out, :] = active.astype(BF)
        scaled[out, :] = (active * w).astype(BF)
        grad_gate[out, :] = (back * up * sig * (1.0 + gate * (1.0 - sig))).astype(BF)
        grad_up[out, :] = (back * silu).astype(BF)
    for n in range(2):
        for c in range(2):
            routed[:, (2 * n + c) * TOK : (2 * n + c + 1) * TOK] = router_rows(pieces[n], c)


def output_kernel(i):
    def kernel(rows, act, grad_gate, grad_up, first, last, out, gain):
        some = slice(i * SLOTS, (i + 1) * SLOTS)
        for b in range(CHIPS):
            cols = slice(b * BK, (b + 1) * BK)
            piece = first.at[EARLY.index(b)] if b in EARLY else last.at[LATE.index(b)]
            out[:, cols] = nt(act[some, :], piece[512:768, :]).astype(BF)
            total = nt(grad_gate[some, :], piece[0:256, :])
            total = total + nt(grad_up[some, :], piece[256:512, :])
            out[:, D + b * BK : D + (b + 1) * BK] = total.astype(BF)
            gain[:, cols] = jnp.sum(total * rows[:, cols].astype(F32), axis=0, keepdims=True)

    return kernel


def grads_kernel(blocks):
    def kernel(flipped, scaled, grad_gate, grad_up, *refs):
        outs, stage, sems = refs[:-2], refs[-2], refs[-1]
        copies = {}
        for n, b in enumerate(blocks):
            slot = n % 3
            if n >= 3:
                copies[n - 3].wait()
            x = flipped[b * BK : (b + 1) * BK, :]
            stage[slot, 0:256, :] = nn(x, grad_gate[...]).astype(BF)
            stage[slot, 256:512, :] = nn(x, grad_up[...]).astype(BF)
            stage[slot, 512:768, :] = nn(
                flipped[D + b * BK : D + (b + 1) * BK, :], scaled[...]
            ).astype(BF)
            copies[n] = pltpu.make_async_copy(stage.at[slot], outs[n], sems.at[slot])
            copies[n].start()
        for n in range(max(0, len(blocks) - 3), len(blocks)):
            copies[n].wait()

    return kernel


def block_of(routed_early, routed_late, b):
    source, n = (routed_early, EARLY.index(b)) if b in EARLY else (routed_late, LATE.index(b))
    return source[:, n * BK : (n + 1) * BK]


def pick_weights(hidden, routed_early, routed_late, chosen):
    logits = jnp.zeros((TOK, 64), F32)
    for b in range(CHIPS):
        r = block_of(routed_early, routed_late, b)
        logits = logits + nt(hidden[:, b * BK : (b + 1) * BK], r)
    raised = jnp.where(chosen[:, :64] > 0.5, jnp.exp(logits), 0.0)
    return raised / jnp.sum(raised, axis=-1, keepdims=True)


def mix_kernel(place, returned, cotangent, spread, chosen, hidden, routed_early, routed_late, gains, gain_mine, gain_other, weight, grad_logits, parts, work):
    w = pick_weights(hidden, routed_early, routed_late, chosen)
    weight[...] = w
    per_slot = jnp.zeros((SLOTS, 1), F32)
    for b in range(CHIPS):
        c = tn(spread[...], cotangent[:, at(place[b] * BK)])
        y = returned[:, b * BK : (b + 1) * BK].astype(F32)
        per_slot = per_slot + jnp.sum(c * y, axis=-1, keepdims=True)
    slot = lax.broadcasted_iota(jnp.int32, (SLOTS, 64), 0)
    who = lax.broadcasted_iota(jnp.int32, (SLOTS, 64), 1)
    spots = jnp.where(who == slot // CAP, per_slot, 0.0)
    high = spots.astype(BF)
    rest = spots - high.astype(F32)
    middle = rest.astype(BF)
    low = (rest - middle.astype(F32)).astype(BF)
    table = spread[...]
    grad_weights = nn(table, high) + nn(table, middle) + nn(table, low)
    inner = jnp.sum(w * grad_weights, axis=-1, keepdims=True)
    g = w * (grad_weights - inner)
    grad_logits[...] = g
    gh, gl = split(g)
    for b in range(CHIPS):
        cols = slice(b * BK, (b + 1) * BK)
        h = hidden[:, cols]
        part = tn(gh, h) + tn(gl, h)
        gain = gain_mine[:, cols] + gain_other[:, cols] + jnp.sum(
            part * block_of(routed_early, routed_late, b).astype(F32), axis=0, keepdims=True
        )
        gain_high, gain_low = split(gain / gains[:, cols])
        for c in range(2):
            home = place[b] * 2 + c
            lanes = slice(c * TOK, (c + 1) * TOK)
            parts[home, 0:64, :] = part[:, lanes].astype(BF)
            work[pl.ds(home, 1), :] = gain_high[:, lanes].astype(F32)
            work[pl.ds(16 + home, 1), :] = gain_low[:, lanes].astype(F32)
    whole = work[...].astype(BF)
    for d in range(16):
        parts[d, 64:96, :] = whole


def norm_kernel(place, returned, spread, weight, grad_logits, routed_early, routed_late, xs, gains, root, mixed, d_tokens, work):
    who = lax.broadcasted_iota(jnp.int32, (64, SLOTS), 0)
    slot = lax.broadcasted_iota(jnp.int32, (64, SLOTS), 1)
    widen = (who == slot // CAP).astype(F32).astype(BF)
    high, low = split(weight[...])
    table = spread[...]
    mask = table.astype(F32)
    blend_high = (nn(high, widen) * mask).astype(BF)
    blend_low = (nn(low, widen) * mask).astype(BF)
    gh, gl = split(grad_logits[...])
    r = root[:, 0:1]
    inner = jnp.zeros((TOK, 1), F32)
    for b in range(CHIPS):
        cols = slice(b * BK, (b + 1) * BK)
        y = returned[:, cols]
        mixed[:, at(place[b] * BK)] = (nn(blend_high, y) + nn(blend_low, y)).astype(BF)
        rt = block_of(routed_early, routed_late, b)
        grad = nn(table, returned[:, D + b * BK : D + (b + 1) * BK]) + nn(gh, rt) + nn(gl, rt)
        scaled = grad * gains[:, cols]
        work[:, cols] = scaled
        inner = inner + jnp.sum(scaled * xs[:, cols].astype(F32), axis=-1, keepdims=True)
    factor = inner * (r * r * r) * (1.0 / D)
    for b in range(CHIPS):
        cols = slice(b * BK, (b + 1) * BK)
        d_tokens[:, at(place[b] * BK)] = (
            work[:, cols] * r - xs[:, cols].astype(F32) * factor
        ).astype(BF)


def total_kernel(place, here, ahead, behind, left, right, give, keep):
    core = place[8]
    for m in range(3):
        for out, side in ((give, 1 - core), (keep, core)):
            rows = at(m * BK + side * TOK, TOK)
            for h, last in enumerate((left, right)):
                cols = slice(h * BK, (h + 1) * BK)
                total = here[rows, cols].astype(F32) + ahead[rows, cols].astype(F32)
                total = total + behind[rows, cols].astype(F32) + last[rows, :].astype(F32)
                out[m * TOK : (m + 1) * TOK, cols] = total.astype(BF)


def share_kernel(parts, shares):
    total = parts[0].astype(F32)
    for d in range(1, 16):
        total = total + parts[d].astype(F32)
    for e in range(WIN):
        shares[e, 0:64, :] = total[0:64]
        shares[e, 64:80, :] = total[64:80] + total[80:96]


def small_kernel(shares, d_router, d_gain):
    total = shares[0]
    for e in range(1, WIN):
        total = total + shares[e]
    d_router[...] = total[0:64]
    d_gain[...] = total[64:80]


def finish_kernel(place, keep, other, *outs):
    core = place[8]
    for m, out in enumerate(outs):
        rows = slice(m * TOK, (m + 1) * TOK)
        out[:, at(core * HALF, HALF)] = keep[rows, :]
        out[:, at((1 - core) * HALF, HALF)] = other[rows, :]


def perm(move):
    pairs = []
    for x in range(2):
        for z in range(4):
            for c in range(2):
                tx, tz, tc = move(x, z, c)
                pairs.append(((x * 4 + z) * 2 + c, (tx * 4 + tz % 4) * 2 + tc))
    return pairs


SIBLING = perm(lambda x, z, c: (x, z, 1 - c))
ACROSS = perm(lambda x, z, c: (1 - x, z, c))
AHEAD = perm(lambda x, z, c: (x, z + 1, c))
BEHIND = perm(lambda x, z, c: (x, z + 3, c))


DP = ("chip", "core")


def send(v, pairs):
    return lax.ppermute(v, DP, pairs)


def gather_pieces(own):
    across = send(own, ACROSS)
    own_1 = send(own, BEHIND)
    own_3 = send(own, AHEAD)
    across_1 = send(across, BEHIND)
    across_3 = send(across, AHEAD)
    own_2 = send(own_3, AHEAD)
    across_2 = send(across_1, BEHIND)
    return (own, own_1, own_2, own_3, across, across_1, across_2, across_3)


def plus(*values):
    total = values[0].astype(F32)
    for v in values[1:]:
        total = total + v.astype(F32)
    return total.astype(BF)


def reduce_pieces(parts):
    cols = [slice(h * BK, (h + 1) * BK) for h in range(2)]
    across_2 = send(parts[6], BEHIND)
    own_2 = send(parts[2], AHEAD)
    across_1 = send(parts[5], AHEAD)
    across_3 = [send(plus(parts[7][:, cols[h]], across_2[:, cols[h]]), BEHIND) for h in range(2)]
    own_3 = send(parts[3], BEHIND)
    own_1 = send(plus(parts[1], own_2), AHEAD)
    across = [send(plus_half(h, parts[4], across_1, across_3[h]), ACROSS) for h in range(2)]
    return parts[0], own_1, own_3, *across


def sum_kernel(h):
    def kernel(*refs):
        sources, out, stage, sems = refs[:-3], refs[-3], refs[-2], refs[-1]
        copies = []
        for n, source in enumerate(sources):
            if source.shape[1] != BK:
                source = source.at[:, h * BK : (h + 1) * BK]
            copies.append(pltpu.make_async_copy(source, stage.at[n], sems.at[n]))
            copies[n].start()
        for c in copies:
            c.wait()
        total = stage[0].astype(F32)
        for n in range(1, len(copies)):
            total = total + stage[n].astype(F32)
        out[...] = total.astype(BF)

    return kernel


def plus_half(h, *values):
    count = len(values)
    return call(
        sum_kernel(h), sds((768, BK), BF), *values, far=range(count), limit=MiB(3),
        scratch=[pltpu.VMEM((count, 768, BK), BF), pltpu.SemaphoreType.DMA((count,))],
    )


def exchange(v, axis):
    return lax.all_to_all(v, axis, split_axis=0, concat_axis=0, tiled=True)


def body(
    tokens, norm_gain, router_weight, expert_ids, gate_weight, up_weight, down_weight, cotangent
):
    chip = lax.axis_index("chip")
    core = lax.axis_index("core")
    x, z = chip >> 2, chip & 3
    rel = jnp.arange(16, dtype=jnp.int32)
    chips = ((x ^ ((rel >> 2) & 1)) * 4 + ((z + rel) & 3)).astype(jnp.int32)
    mine = jnp.where(rel == 8, core, lax.axis_index("expert")).astype(jnp.int32)
    place = jnp.where(rel < 8, chips, mine)

    weights = (gate_weight[0], up_weight[0], down_weight[0])
    away, keep_own = call(
        pack_kernel, [sds((400, HALF), BF)] * 2, place, *weights, router_weight.T, smem=1,
        limit=MiB(2), far=(1, 2, 3), scratch=[pltpu.SemaphoreType.DMA((2, 3))],
    )
    other = send(away, SIBLING)
    hidden, xs, gains, root, spread, chosen, sent = call(
        dispatch_kernel,
        [pltpu.HBM((TOK, D), BF), pltpu.HBM((TOK, D), BF), pltpu.HBM((1, D), F32),
         pltpu.HBM((TOK, 128), F32), pltpu.HBM((TOK, SLOTS), BF), pltpu.HBM((TOK, 128), F32),
         pltpu.HBM((SLOTS, WIDE), BF)],
        place, tokens, cotangent, norm_gain[None], expert_ids, smem=1, dram=(1, 2, 3),
        limit=MiB(12),
    )
    own = call(join_kernel, sds((ROWS, HALF), BF), place, keep_own, other, smem=1, limit=MiB(3))
    pieces = gather_pieces(own)

    rows = exchange(sent.reshape(WIN, CAP, WIDE), "expert").reshape(SLOTS, WIDE)
    rows_other = send(rows, SIBLING)
    flipped = call(flip_kernel, sds((2 * D, 2 * SLOTS), BF), rows, rows_other, limit=MiB(12))
    shapes = [sds((SLOTS, 3 * HALF), F32), sds((SLOTS, 64), F32)]
    sums, slot_logits, routed_early, held_early = call(
        early_kernel,
        shapes + [pltpu.HBM((64, 6 * BK), BF), pltpu.VMEM((6, ROWS, HALF), BF)],
        rows, *[pieces[b] for b in EARLY], limit=MiB(6), far=range(1, 7),
        scratch=[pltpu.SemaphoreType.DMA((6,))],
    )
    sums_other, logits_other = call(
        early_other_kernel, shapes, rows_other, held_early, limit=MiB(6),
    )
    act, scaled, grad_gate, grad_up, routed_late, held_late = call(
        late_kernel,
        [sds((2 * SLOTS, HALF), BF)] * 4
        + [pltpu.HBM((64, 2 * BK), BF), pltpu.VMEM((2, ROWS, HALF), BF)],
        place, rows, sums, slot_logits, rows_other, sums_other, logits_other,
        *[pieces[b] for b in LATE], smem=1, limit=MiB(8), far=(7, 8),
        scratch=[pltpu.SemaphoreType.DMA((2,))],
    )
    (partial_other, gain_other), (partial, gain_mine) = (
        call(
            output_kernel(i), [sds((SLOTS, 2 * D), BF), sds((1, D), F32)],
            source, act, grad_gate, grad_up, held_early, held_late, limit=MiB(6),
        )
        for i, source in ((1, rows_other), (0, rows))
    )
    output = plus(partial, send(partial_other, SIBLING))
    returned = exchange(output.reshape(WIN, CAP, 2 * D), "expert")
    returned = returned.reshape(SLOTS, 2 * D)
    parts = {}
    for blocks in ((6, 2, 5), (7, 3, 1, 4, 0)):
        made = call(
            grads_kernel(blocks), [pltpu.HBM((768, HALF), BF)] * len(blocks),
            flipped, scaled, grad_gate, grad_up, limit=MiB(5), far_out=True,
            scratch=[pltpu.VMEM((3, 768, HALF), BF), pltpu.SemaphoreType.DMA((3,))],
        )
        parts.update(zip(blocks, made))
    give, keep = call(
        total_kernel, [sds((384, HALF), BF)] * 2, place, *reduce_pieces(parts),
        smem=1, limit=MiB(6),
    )
    fetched = send(give, SIBLING)
    d_weights = call(
        finish_kernel, [pltpu.HBM((TOK, FF), BF)] * 3, place, keep, fetched,
        smem=1, limit=MiB(4),
    )

    weight, grad_logits, shares = call(
        mix_kernel,
        [sds((TOK, 64), F32), sds((TOK, 64), F32), pltpu.HBM((16, 96, TOK), BF)],
        place, returned, cotangent, spread, chosen, hidden, routed_early, routed_late, gains,
        gain_mine, gain_other, smem=1, dram=range(2, 9), limit=MiB(12),
        scratch=[pltpu.VMEM((32, TOK), F32)],
    )
    shares = exchange(shares, DP)
    shares = call(share_kernel, sds((8, 80, TOK), F32), shares, limit=MiB(2))
    shares = exchange(shares, "expert")
    d_router, d_gain = call(
        small_kernel, [pltpu.HBM((64, TOK), F32), pltpu.HBM((16, TOK), F32)], shares, limit=MiB(2)
    )

    mixed, d_tokens = call(
        norm_kernel, [pltpu.HBM((TOK, D), BF)] * 2,
        place, returned, spread, weight, grad_logits, routed_early, routed_late, xs, gains, root,
        smem=1, dram=(2, 5, 6, 7, 8, 9), limit=MiB(10), scratch=[pltpu.VMEM((TOK, D), F32)],
    )
    return (mixed, d_tokens, d_gain.reshape(D), d_router.T, *[d[None] for d in d_weights])


def MiB(n):
    return n << 20


def solution(mesh):
    grid = Mesh(mesh.devices.reshape(8, 2, 8), ("chip", "core", "expert"))
    every = P(("chip", "core", "expert"), None)
    rows = P("expert", DP, None)
    in_specs = (every, P(), P(DP, None), every, rows, rows, rows, every)
    out_specs = (every, every, P(), P(DP, None), rows, rows, rows)
    return jax.shard_map(body, mesh=grid, in_specs=in_specs, out_specs=out_specs, check_vma=False)
```

```python
import jax
import jax.numpy as jnp
from jax import lax
from jax.experimental import pallas as pl
from jax.experimental.pallas import tpu as pltpu
from jax.sharding import Mesh
from jax.sharding import PartitionSpec as P


D = 2048
FF = 1024
CAP = 32
TOK = 128
WIN = 8
SLOTS = WIN * CAP
EPSILON = 1e-05
BK = 256
HALF = 512
WIDE = 2 * D + 128
ROWS = 800
CHIPS = 8
LEFT, RIGHT = slice(0, BK), slice(BK, HALF)
SIDES = (LEFT, RIGHT)
F32 = jnp.float32
BF = jnp.bfloat16


def nn(a, b):
    return lax.dot_general(a, b, (((1,), (0,)), ((), ())), preferred_element_type=F32)


def nt(a, b):
    return lax.dot_general(a, b, (((1,), (1,)), ((), ())), preferred_element_type=F32)


def tn(a, b):
    return lax.dot_general(a, b, (((0,), (0,)), ((), ())), preferred_element_type=F32)


def split(v):
    high = v.astype(BF)
    return high, (v - high.astype(F32)).astype(BF)


def sds(shape, dtype):
    return jax.ShapeDtypeStruct(shape, dtype)


SMEM = pl.BlockSpec(memory_space=pltpu.SMEM)
VMEM = pl.BlockSpec(memory_space=pltpu.VMEM)
HBM = pl.BlockSpec(memory_space=pltpu.HBM)


def call(kernel, out_shape, *args, smem=0, near=True, limit=None, scratch=(), far=(), dram=(), far_out=False):
    outs = out_shape if isinstance(out_shape, (list, tuple)) else [out_shape]
    specs = [SMEM] * smem + [VMEM] * (len(args) - smem)
    for i in far:
        specs[i] = HBM
    out_spec = HBM if far_out else VMEM
    if near:
        args = args[:smem] + tuple(
            pltpu.with_memory_space_constraint(v, pltpu.HBM) if i + smem in far or i + smem in dram else pltpu.with_memory_space_constraint(v, pltpu.VMEM)
            for i, v in enumerate(args[smem:])
        )
    params = pltpu.CompilerParams(vmem_limit_bytes=limit) if limit else None
    return pl.pallas_call(
        kernel,
        out_shape=out_shape,
        in_specs=specs,
        out_specs=[out_spec] * len(outs) if isinstance(out_shape, (list, tuple)) else out_spec,
        scratch_shapes=list(scratch),
        compiler_params=params,
    )(*args)


def at(ref_index, block=BK):
    return pl.ds(pl.multiple_of(ref_index, block), block)


def pack_kernel(place, gate, up, down, router_t, away, keep, sems):
    copies = []
    for m, w in enumerate((gate, up, down)):
        for j, (out, side) in enumerate(((away, 1 - place[8]), (keep, place[8]))):
            copies.append(
                pltpu.make_async_copy(
                    w.at[:, at(side * HALF, HALF)], out.at[m * TOK : (m + 1) * TOK, :], sems.at[j, m]
                )
            )
    for c in copies:
        c.start()
    for g in range(4):
        for out in (away, keep):
            out[384:400, g * TOK : (g + 1) * TOK] = router_t[g * 16 : (g + 1) * 16, :]
    for c in copies:
        c.wait()


def join_kernel(place, keep, other, own):
    core = place[8]
    for source, side in ((keep, core), (other, 1 - core)):
        for m in range(3):
            own[at(m * BK + side * TOK, TOK), :] = source[m * TOK : (m + 1) * TOK, :]
        own[at(768 + side * 16, 16), :] = source[384:400, :]


def router_rows(piece, c):
    rows = piece[768 + c * 16 : 784 + c * 16, :]
    return jnp.concatenate([rows[:, g * TOK : (g + 1) * TOK] for g in range(4)], axis=0)


def dispatch_kernel(place, tokens, cotangent, gain, ids, hidden, xs, gains, root, spread, chosen, outgoing):
    lane = lax.broadcasted_iota(jnp.int32, (TOK, 128), 1)
    picked = jnp.zeros((TOK, 128), F32)
    for k in range(8):
        picked = picked + (ids[:, k : k + 1] == lane).astype(F32)
    chosen[...] = picked
    half = picked.astype(BF)
    row = lax.broadcasted_iota(jnp.int32, (TOK, TOK), 0)
    col = lax.broadcasted_iota(jnp.int32, (TOK, TOK), 1)
    earlier = nn((col < row).astype(F32).astype(BF), half)
    who = lax.broadcasted_iota(jnp.int32, (128, SLOTS), 0)
    slot = lax.broadcasted_iota(jnp.int32, (128, SLOTS), 1)
    widen = (who == slot // CAP).astype(F32).astype(BF)
    position = nn(earlier.astype(BF), widen)
    named = nn(half, widen)
    column = lax.broadcasted_iota(jnp.int32, (TOK, SLOTS), 1)
    table = jnp.where(
        (named > 0.5) & (position == (column % CAP).astype(F32)), 1.0, 0.0
    ).astype(BF)
    spread[...] = table
    total = jnp.zeros((TOK, 1), F32)
    for b in range(CHIPS):
        x = tokens[:, at(place[b] * BK)]
        xs[:, b * BK : (b + 1) * BK] = x
        x = x.astype(F32)
        total = total + jnp.sum(x * x, axis=-1, keepdims=True)
    r = lax.rsqrt(total * (1.0 / D) + EPSILON)
    root[...] = jnp.broadcast_to(r, (TOK, 128))
    for b in range(CHIPS):
        cols = slice(b * BK, (b + 1) * BK)
        g = gain[:, at(place[b] * BK)]
        gains[:, cols] = g
        h = (xs[:, cols].astype(F32) * r * g).astype(BF)
        hidden[:, cols] = h
        outgoing[:, cols] = tn(table, h).astype(BF)
        outgoing[:, D + b * BK : D + (b + 1) * BK] = tn(
            table, cotangent[:, at(place[b] * BK)]
        ).astype(BF)
    outgoing[:, 2 * D :] = tn(table, half).astype(BF)


def flip_kernel(mine, other, flipped):
    for b in range(16):
        cols = slice(b * BK, (b + 1) * BK)
        flipped[cols, 0:SLOTS] = mine[:, cols].T
        flipped[cols, SLOTS : 2 * SLOTS] = other[:, cols].T


EARLY = (0, 1, 3, 4, 2, 5)
LATE = (7, 6)


def products(rows, pieces, blocks, totals, logits):
    for b, piece in zip(blocks, pieces):
        x = rows[:, b * BK : (b + 1) * BK]
        y = rows[:, D + b * BK : D + (b + 1) * BK]
        totals[0] = totals[0] + nn(x, piece[0:256, :])
        totals[1] = totals[1] + nn(x, piece[256:512, :])
        totals[2] = totals[2] + nn(y, piece[512:768, :])
        for c in range(2):
            logits = logits + nt(x[:, c * TOK : (c + 1) * TOK], router_rows(piece, c))
    return totals, logits


def fetch(sources, held, sems):
    copies = []
    for n, source in enumerate(sources):
        for h, part in enumerate(source):
            target = held.at[n] if len(source) == 1 else held.at[n, :, SIDES[h]]
            copies.append(pltpu.make_async_copy(part, target, sems.at[n, h]))
    for c in copies:
        c.start()
    for c in copies:
        c.wait()
    return [held.at[n] for n in range(len(sources))]


def keep_products(rows, pieces, sums, slot_logits):
    totals, logits = products(
        rows, pieces, EARLY, [jnp.zeros((SLOTS, HALF), F32)] * 3, jnp.zeros((SLOTS, 64), F32)
    )
    for m in range(3):
        sums[:, m * HALF : (m + 1) * HALF] = totals[m]
    slot_logits[...] = logits


def early_kernel(rows, *refs):
    sums, slot_logits, routed, held, sems = refs[7:]
    pieces = fetch([refs[n : n + 1] for n in range(5)] + [refs[5:7]], held, sems)
    keep_products(rows, pieces, sums, slot_logits)
    for n in range(6):
        for c in range(2):
            routed[:, (2 * n + c) * TOK : (2 * n + c + 1) * TOK] = router_rows(pieces[n], c)


def early_other_kernel(rows, held, sums, slot_logits):
    keep_products(rows, [held.at[n] for n in range(6)], sums, slot_logits)


def late_kernel(place, *refs):
    act, scaled, grad_gate, grad_up, routed, held, sems = refs[9:]
    pieces = fetch([refs[6:7], refs[7:9]], held, sems)
    lane = lax.broadcasted_iota(jnp.int32, (SLOTS, 64), 1)
    for i in range(2):
        rows, sums, slot_logits = refs[3 * i : 3 * i + 3]
        out = slice(i * SLOTS, (i + 1) * SLOTS)
        totals, logits = products(
            rows, pieces, LATE, [sums[:, m * HALF : (m + 1) * HALF] for m in range(3)],
            slot_logits[...],
        )
        picked = rows[:, 2 * D : 2 * D + 64].astype(F32) > 0.5
        raised = jnp.where(picked, jnp.exp(logits), 0.0)
        mine = jnp.sum(jnp.where(lane == place[9], raised, 0.0), axis=-1, keepdims=True)
        total = jnp.sum(raised, axis=-1, keepdims=True)
        w = jnp.where(total > 0.0, mine / jnp.where(total > 0.0, total, 1.0), 0.0)
        gate, up, back = totals
        sig = jax.nn.sigmoid(gate)
        silu = gate * sig
        active = silu * up
        back = back * w
        act[out, :] = active.astype(BF)
        scaled[out, :] = (active * w).astype(BF)
        grad_gate[out, :] = (back * up * sig * (1.0 + gate * (1.0 - sig))).astype(BF)
        grad_up[out, :] = (back * silu).astype(BF)
    for n in range(2):
        for c in range(2):
            routed[:, (2 * n + c) * TOK : (2 * n + c + 1) * TOK] = router_rows(pieces[n], c)


def output_kernel(i):
    def kernel(rows, act, grad_gate, grad_up, first, last, *refs):
        out, gain = refs[-2:]
        some = slice(i * SLOTS, (i + 1) * SLOTS)
        for b in range(CHIPS):
            cols = slice(b * BK, (b + 1) * BK)
            more = slice(D + b * BK, D + (b + 1) * BK)
            piece = first.at[EARLY.index(b)] if b in EARLY else last.at[LATE.index(b)]
            made = nt(act[some, :], piece[512:768, :])
            total = nt(grad_gate[some, :], piece[0:256, :])
            total = total + nt(grad_up[some, :], piece[256:512, :])
            gain[:, cols] = jnp.sum(total * rows[:, cols].astype(F32), axis=0, keepdims=True)
            if len(refs) == 3:
                made = made + refs[0][:, cols].astype(F32)
                total = total + refs[0][:, more].astype(F32)
            out[:, cols] = made.astype(BF)
            out[:, more] = total.astype(BF)

    return kernel


def grads_kernel(blocks):
    def kernel(flipped, scaled, grad_gate, grad_up, *refs):
        outs, stage, sems = refs[:-2], refs[-2], refs[-1]
        copies = {}
        for n, b in enumerate(blocks):
            slot = n % 3
            if n >= 3:
                for c in copies[n - 3]:
                    c.wait()
            x = flipped[b * BK : (b + 1) * BK, :]
            stage[slot, 0:256, :] = nn(x, grad_gate[...]).astype(BF)
            stage[slot, 256:512, :] = nn(x, grad_up[...]).astype(BF)
            stage[slot, 512:768, :] = nn(
                flipped[D + b * BK : D + (b + 1) * BK, :], scaled[...]
            ).astype(BF)
            if b == 3:
                copies[n] = [
                    pltpu.make_async_copy(stage.at[slot, :, side], out, sems.at[slot, h])
                    for h, (side, out) in enumerate(zip(SIDES, (outs[n], outs[-1])))
                ]
            else:
                copies[n] = [pltpu.make_async_copy(stage.at[slot], outs[n], sems.at[slot, 0])]
            for c in copies[n]:
                c.start()
        for n in range(max(0, len(blocks) - 3), len(blocks)):
            for c in copies[n]:
                c.wait()

    return kernel


def block_of(routed_early, routed_late, b):
    source, n = (routed_early, EARLY.index(b)) if b in EARLY else (routed_late, LATE.index(b))
    return source[:, n * BK : (n + 1) * BK]


def pick_weights(hidden, routed_early, routed_late, chosen):
    logits = jnp.zeros((TOK, 64), F32)
    for b in range(CHIPS):
        r = block_of(routed_early, routed_late, b)
        logits = logits + nt(hidden[:, b * BK : (b + 1) * BK], r)
    raised = jnp.where(chosen[:, :64] > 0.5, jnp.exp(logits), 0.0)
    return raised / jnp.sum(raised, axis=-1, keepdims=True)


def mix_kernel(place, returned, cotangent, spread, chosen, hidden, routed_early, routed_late, gains, gain_mine, gain_other, weight, grad_logits, parts, work):
    w = pick_weights(hidden, routed_early, routed_late, chosen)
    weight[...] = w
    per_slot = jnp.zeros((SLOTS, 1), F32)
    for b in range(CHIPS):
        c = tn(spread[...], cotangent[:, at(place[b] * BK)])
        y = returned[:, b * BK : (b + 1) * BK].astype(F32)
        per_slot = per_slot + jnp.sum(c * y, axis=-1, keepdims=True)
    slot = lax.broadcasted_iota(jnp.int32, (SLOTS, 64), 0)
    who = lax.broadcasted_iota(jnp.int32, (SLOTS, 64), 1)
    spots = jnp.where(who == slot // CAP, per_slot, 0.0)
    high = spots.astype(BF)
    rest = spots - high.astype(F32)
    middle = rest.astype(BF)
    low = (rest - middle.astype(F32)).astype(BF)
    table = spread[...]
    grad_weights = nn(table, high) + nn(table, middle) + nn(table, low)
    inner = jnp.sum(w * grad_weights, axis=-1, keepdims=True)
    g = w * (grad_weights - inner)
    grad_logits[...] = g
    gh, gl = split(g)
    for b in range(CHIPS):
        cols = slice(b * BK, (b + 1) * BK)
        h = hidden[:, cols]
        part = tn(gh, h) + tn(gl, h)
        gain = gain_mine[:, cols] + gain_other[:, cols] + jnp.sum(
            part * block_of(routed_early, routed_late, b).astype(F32), axis=0, keepdims=True
        )
        gain_high, gain_low = split(gain / gains[:, cols])
        for c in range(2):
            home = place[b] * 2 + c
            lanes = slice(c * TOK, (c + 1) * TOK)
            parts[home, 0:64, :] = part[:, lanes].astype(BF)
            work[pl.ds(home, 1), :] = gain_high[:, lanes].astype(F32)
            work[pl.ds(16 + home, 1), :] = gain_low[:, lanes].astype(F32)
    whole = work[...].astype(BF)
    for d in range(16):
        parts[d, 64:96, :] = whole


def norm_kernel(place, returned, spread, weight, grad_logits, routed_early, routed_late, xs, gains, root, mixed, d_tokens, work):
    who = lax.broadcasted_iota(jnp.int32, (64, SLOTS), 0)
    slot = lax.broadcasted_iota(jnp.int32, (64, SLOTS), 1)
    widen = (who == slot // CAP).astype(F32).astype(BF)
    high, low = split(weight[...])
    table = spread[...]
    mask = table.astype(F32)
    blend_high = (nn(high, widen) * mask).astype(BF)
    blend_low = (nn(low, widen) * mask).astype(BF)
    gh, gl = split(grad_logits[...])
    r = root[:, 0:1]
    inner = jnp.zeros((TOK, 1), F32)
    for b in range(CHIPS):
        cols = slice(b * BK, (b + 1) * BK)
        y = returned[:, cols]
        mixed[:, at(place[b] * BK)] = (nn(blend_high, y) + nn(blend_low, y)).astype(BF)
        rt = block_of(routed_early, routed_late, b)
        grad = nn(table, returned[:, D + b * BK : D + (b + 1) * BK]) + nn(gh, rt) + nn(gl, rt)
        scaled = grad * gains[:, cols]
        work[:, cols] = scaled
        inner = inner + jnp.sum(scaled * xs[:, cols].astype(F32), axis=-1, keepdims=True)
    factor = inner * (r * r * r) * (1.0 / D)
    for b in range(CHIPS):
        cols = slice(b * BK, (b + 1) * BK)
        d_tokens[:, at(place[b] * BK)] = (
            work[:, cols] * r - xs[:, cols].astype(F32) * factor
        ).astype(BF)


def total_kernel(place, here, *refs):
    halves, give, keep = refs[:6], refs[6], refs[7]
    core = place[8]
    for m in range(3):
        for out, side in ((give, 1 - core), (keep, core)):
            rows = at(m * BK + side * TOK, TOK)
            for h, cols in enumerate(SIDES):
                total = here[rows, cols].astype(F32)
                for v in halves[h::2]:
                    total = total + v[rows, :].astype(F32)
                out[m * TOK : (m + 1) * TOK, cols] = total.astype(BF)


def share_kernel(parts, shares):
    total = parts[0].astype(F32)
    for d in range(1, 16):
        total = total + parts[d].astype(F32)
    for e in range(WIN):
        shares[e, 0:64, :] = total[0:64]
        shares[e, 64:80, :] = total[64:80] + total[80:96]


def small_kernel(shares, d_router, d_gain):
    total = shares[0]
    for e in range(1, WIN):
        total = total + shares[e]
    d_router[...] = total[0:64]
    d_gain[...] = total[64:80]


def finish_kernel(place, keep, other, *outs):
    core = place[8]
    for m, out in enumerate(outs):
        rows = slice(m * TOK, (m + 1) * TOK)
        out[:, at(core * HALF, HALF)] = keep[rows, :]
        out[:, at((1 - core) * HALF, HALF)] = other[rows, :]


def perm(move):
    pairs = []
    for x in range(2):
        for z in range(4):
            for c in range(2):
                tx, tz, tc = move(x, z, c)
                pairs.append(((x * 4 + z) * 2 + c, (tx * 4 + tz % 4) * 2 + tc))
    return pairs


SIBLING = perm(lambda x, z, c: (x, z, 1 - c))
ACROSS = perm(lambda x, z, c: (1 - x, z, c))
AHEAD = perm(lambda x, z, c: (x, z + 1, c))
BEHIND = perm(lambda x, z, c: (x, z + 3, c))


DP = ("chip", "core")


def send(v, pairs):
    return lax.ppermute(v, DP, pairs)


def gather_pieces(own):
    across = send(own, ACROSS)
    own_3 = send(own, AHEAD)
    own_1 = send(own, BEHIND)
    own_2 = send(own_3, AHEAD)
    across_1 = [send(across[:, side], BEHIND) for side in SIDES]
    across_3 = send(across, AHEAD)
    across_2 = [send(v, BEHIND) for v in across_1]
    return ([own], [own_1], [own_2], [own_3], [across], across_1, across_2, [across_3])


def plus(*values):
    total = values[0].astype(F32)
    for v in values[1:]:
        total = total + v.astype(F32)
    return total.astype(BF)


def reduce_pieces(parts):
    across_2 = send(parts[6], BEHIND)
    across_1 = send(parts[5], AHEAD)
    own_2 = send(parts[2], AHEAD)
    across_3 = [send(plus(parts[7][:, side], across_2[:, side]), BEHIND) for side in SIDES]
    own_3 = [send(v, BEHIND) for v in (parts[3], parts[8])]
    own_1 = [send(plus(parts[1][:, side], own_2[:, side]), AHEAD) for side in SIDES]
    across = [
        send(v, ACROSS)
        for v in (
            plus(parts[4][:, LEFT], across_1[:, LEFT], across_3[0]),
            plus_half(1, parts[4], across_1, across_3[1]),
        )
    ]
    return parts[0], *own_1, *own_3, *across


def sum_kernel(h):
    def kernel(*refs):
        sources, out, stage, sems = refs[:-3], refs[-3], refs[-2], refs[-1]
        copies = []
        for n, source in enumerate(sources):
            if source.shape[1] != BK:
                source = source.at[:, h * BK : (h + 1) * BK]
            copies.append(pltpu.make_async_copy(source, stage.at[n], sems.at[n]))
            copies[n].start()
        for c in copies:
            c.wait()
        total = stage[0].astype(F32)
        for n in range(1, len(copies)):
            total = total + stage[n].astype(F32)
        out[...] = total.astype(BF)

    return kernel


def plus_half(h, *values):
    count = len(values)
    return call(
        sum_kernel(h), sds((768, BK), BF), *values, far=range(count), limit=MiB(3),
        scratch=[pltpu.VMEM((count, 768, BK), BF), pltpu.SemaphoreType.DMA((count,))],
    )


def exchange(v, axis):
    return lax.all_to_all(v, axis, split_axis=0, concat_axis=0, tiled=True)


def body(
    tokens, norm_gain, router_weight, expert_ids, gate_weight, up_weight, down_weight, cotangent
):
    chip = lax.axis_index("chip")
    core = lax.axis_index("core")
    x, z = chip >> 2, chip & 3
    rel = jnp.arange(16, dtype=jnp.int32)
    chips = ((x ^ ((rel >> 2) & 1)) * 4 + ((z + rel) & 3)).astype(jnp.int32)
    mine = jnp.where(rel == 8, core, lax.axis_index("expert")).astype(jnp.int32)
    place = jnp.where(rel < 8, chips, mine)

    weights = (gate_weight[0], up_weight[0], down_weight[0])
    away, keep_own = call(
        pack_kernel, [sds((400, HALF), BF)] * 2, place, *weights, router_weight.T, smem=1,
        limit=MiB(2), far=(1, 2, 3), dram=(4,), scratch=[pltpu.SemaphoreType.DMA((2, 3))],
    )
    other = send(away, SIBLING)
    hidden, xs, gains, root, spread, chosen, sent = call(
        dispatch_kernel,
        [pltpu.HBM((TOK, D), BF), pltpu.HBM((TOK, D), BF), pltpu.HBM((1, D), F32),
         pltpu.HBM((TOK, 128), F32), pltpu.HBM((TOK, SLOTS), BF), pltpu.HBM((TOK, 128), F32),
         pltpu.HBM((SLOTS, WIDE), BF)],
        place, tokens, cotangent, norm_gain[None], expert_ids, smem=1, dram=(1, 2, 3),
        limit=MiB(12),
    )
    own = call(join_kernel, sds((ROWS, HALF), BF), place, keep_own, other, smem=1, limit=MiB(3))
    pieces = gather_pieces(own)

    rows = exchange(sent.reshape(WIN, CAP, WIDE), "expert").reshape(SLOTS, WIDE)
    rows_other = send(rows, SIBLING)
    flipped = call(flip_kernel, sds((2 * D, 2 * SLOTS), BF), rows, rows_other, limit=MiB(12))
    shapes = [sds((SLOTS, 3 * HALF), F32), sds((SLOTS, 64), F32)]
    sums, slot_logits, routed_early, held_early = call(
        early_kernel,
        shapes + [pltpu.HBM((64, 6 * BK), BF), pltpu.VMEM((6, ROWS, HALF), BF)],
        rows, *[v for b in EARLY for v in pieces[b]], limit=MiB(6), far=range(1, 8),
        scratch=[pltpu.SemaphoreType.DMA((6, 2))],
    )
    sums_other, logits_other = call(
        early_other_kernel, shapes, rows_other, held_early, limit=MiB(6),
    )
    act, scaled, grad_gate, grad_up, routed_late, held_late = call(
        late_kernel,
        [sds((2 * SLOTS, HALF), BF)] * 4
        + [pltpu.HBM((64, 2 * BK), BF), pltpu.VMEM((2, ROWS, HALF), BF)],
        place, rows, sums, slot_logits, rows_other, sums_other, logits_other,
        *[v for b in LATE for v in pieces[b]], smem=1, limit=MiB(8), far=(7, 8, 9),
        scratch=[pltpu.SemaphoreType.DMA((2, 2))],
    )
    shapes = [sds((SLOTS, 2 * D), BF), sds((1, D), F32)]
    operands = (act, grad_gate, grad_up, held_early, held_late)
    partial, gain_other = call(output_kernel(1), shapes, rows_other, *operands, limit=MiB(6))
    received = send(partial, SIBLING)
    output, gain_mine = call(output_kernel(0), shapes, rows, *operands, received, limit=MiB(8))
    returned = exchange(output.reshape(WIN, CAP, 2 * D), "expert")
    returned = returned.reshape(SLOTS, 2 * D)
    parts = {}
    for blocks in ((6, 5, 2), (3, 7, 1, 4, 0)):
        shapes = [pltpu.HBM((768, BK if b == 3 else HALF), BF) for b in blocks]
        if 3 in blocks:
            shapes.append(pltpu.HBM((768, BK), BF))
        made = call(
            grads_kernel(blocks), shapes, flipped, scaled, grad_gate, grad_up,
            limit=MiB(5), far_out=True,
            scratch=[pltpu.VMEM((3, 768, HALF), BF), pltpu.SemaphoreType.DMA((3, 2))],
        )
        parts.update(zip(blocks + (8,), made))
    give, keep = call(
        total_kernel, [sds((384, HALF), BF)] * 2, place, *reduce_pieces(parts),
        smem=1, limit=MiB(6),
    )
    fetched = send(give, SIBLING)
    d_weights = call(
        finish_kernel, [pltpu.HBM((TOK, FF), BF)] * 3, place, keep, fetched,
        smem=1, limit=MiB(4),
    )

    weight, grad_logits, shares = call(
        mix_kernel,
        [sds((TOK, 64), F32), sds((TOK, 64), F32), pltpu.HBM((16, 96, TOK), BF)],
        place, returned, cotangent, spread, chosen, hidden, routed_early, routed_late, gains,
        gain_mine, gain_other, smem=1, dram=range(2, 9), limit=MiB(12),
        scratch=[pltpu.VMEM((32, TOK), F32)],
    )
    shares = exchange(shares, DP)
    shares = call(share_kernel, sds((8, 80, TOK), F32), shares, limit=MiB(2))
    shares = exchange(shares, "expert")
    d_router, d_gain = call(
        small_kernel, [pltpu.HBM((64, TOK), F32), pltpu.HBM((16, TOK), F32)], shares, limit=MiB(2)
    )

    mixed, d_tokens = call(
        norm_kernel, [pltpu.HBM((TOK, D), BF)] * 2,
        place, returned, spread, weight, grad_logits, routed_early, routed_late, xs, gains, root,
        smem=1, dram=(2, 5, 6, 7, 8, 9), limit=MiB(10), scratch=[pltpu.VMEM((TOK, D), F32)],
    )
    return (mixed, d_tokens, d_gain.reshape(D), d_router.T, *[d[None] for d in d_weights])


def MiB(n):
    return n << 20


def solution(mesh):
    grid = Mesh(mesh.devices.reshape(8, 2, 8), ("chip", "core", "expert"))
    every = P(("chip", "core", "expert"), None)
    rows = P("expert", DP, None)
    in_specs = (every, P(), P(DP, None), every, rows, rows, rows, every)
    out_specs = (every, every, P(), P(DP, None), rows, rows, rows)
    return jax.shard_map(body, mesh=grid, in_specs=in_specs, out_specs=out_specs, check_vma=False)
```

```python
import jax
import jax.numpy as jnp
from jax import lax
from jax.experimental import pallas as pl
from jax.experimental.pallas import tpu as pltpu
from jax.sharding import Mesh
from jax.sharding import PartitionSpec as P


D = 2048
FF = 1024
CAP = 32
TOK = 128
WIN = 8
SLOTS = WIN * CAP
EPSILON = 1e-05
BK = 256
HALF = 512
WIDE = 2 * D + 128
ROWS = 800
CHIPS = 8
LEFT, RIGHT = slice(0, BK), slice(BK, HALF)
SIDES = (LEFT, RIGHT)
F32 = jnp.float32
BF = jnp.bfloat16


def nn(a, b):
    return lax.dot_general(a, b, (((1,), (0,)), ((), ())), preferred_element_type=F32)


def nt(a, b):
    return lax.dot_general(a, b, (((1,), (1,)), ((), ())), preferred_element_type=F32)


def tn(a, b):
    return lax.dot_general(a, b, (((0,), (0,)), ((), ())), preferred_element_type=F32)


def split(v):
    high = v.astype(BF)
    return high, (v - high.astype(F32)).astype(BF)


def sds(shape, dtype):
    return jax.ShapeDtypeStruct(shape, dtype)


SMEM = pl.BlockSpec(memory_space=pltpu.SMEM)
VMEM = pl.BlockSpec(memory_space=pltpu.VMEM)
HBM = pl.BlockSpec(memory_space=pltpu.HBM)


def call(kernel, out_shape, *args, smem=0, near=True, limit=None, scratch=(), far=(), dram=(), far_out=False, out_specs=None):
    outs = out_shape if isinstance(out_shape, (list, tuple)) else [out_shape]
    specs = [SMEM] * smem + [VMEM] * (len(args) - smem)
    for i in far:
        specs[i] = HBM
    out_spec = HBM if far_out else VMEM
    if near:
        args = args[:smem] + tuple(
            pltpu.with_memory_space_constraint(v, pltpu.HBM) if i + smem in far or i + smem in dram else pltpu.with_memory_space_constraint(v, pltpu.VMEM)
            for i, v in enumerate(args[smem:])
        )
    params = pltpu.CompilerParams(vmem_limit_bytes=limit) if limit else None
    return pl.pallas_call(
        kernel,
        out_shape=out_shape,
        in_specs=specs,
        out_specs=out_specs or [out_spec] * len(outs) if isinstance(out_shape, (list, tuple)) else out_spec,
        scratch_shapes=list(scratch),
        compiler_params=params,
    )(*args)


def at(ref_index, block=BK):
    return pl.ds(pl.multiple_of(ref_index, block), block)


def pack_kernel(place, gate, up, down, router_t, away, keep, sems):
    copies = []
    for m, w in enumerate((gate, up, down)):
        for j, (out, side) in enumerate(((away, 1 - place[8]), (keep, place[8]))):
            copies.append(
                pltpu.make_async_copy(
                    w.at[:, at(side * HALF, HALF)], out.at[m * TOK : (m + 1) * TOK, :], sems.at[j, m]
                )
            )
    for c in copies:
        c.start()
    for g in range(4):
        for out in (away, keep):
            out[384:400, g * TOK : (g + 1) * TOK] = router_t[g * 16 : (g + 1) * 16, :]
    for c in copies:
        c.wait()


def join_kernel(place, keep, other, own):
    core = place[8]
    for source, side in ((keep, core), (other, 1 - core)):
        for m in range(3):
            own[at(m * BK + side * TOK, TOK), :] = source[m * TOK : (m + 1) * TOK, :]
        own[at(768 + side * 16, 16), :] = source[384:400, :]


def router_rows(piece, c):
    rows = piece[768 + c * 16 : 784 + c * 16, :]
    return jnp.concatenate([rows[:, g * TOK : (g + 1) * TOK] for g in range(4)], axis=0)


def dispatch_kernel(place, tokens, cotangent, gain, ids, hidden, xs, gains, root, spread, chosen, outgoing):
    lane = lax.broadcasted_iota(jnp.int32, (TOK, 128), 1)
    picked = jnp.zeros((TOK, 128), F32)
    for k in range(8):
        picked = picked + (ids[:, k : k + 1] == lane).astype(F32)
    chosen[...] = picked
    half = picked.astype(BF)
    row = lax.broadcasted_iota(jnp.int32, (TOK, TOK), 0)
    col = lax.broadcasted_iota(jnp.int32, (TOK, TOK), 1)
    earlier = nn((col < row).astype(F32).astype(BF), half)
    who = lax.broadcasted_iota(jnp.int32, (128, SLOTS), 0)
    slot = lax.broadcasted_iota(jnp.int32, (128, SLOTS), 1)
    widen = (who == slot // CAP).astype(F32).astype(BF)
    position = nn(earlier.astype(BF), widen)
    named = nn(half, widen)
    column = lax.broadcasted_iota(jnp.int32, (TOK, SLOTS), 1)
    table = jnp.where(
        (named > 0.5) & (position == (column % CAP).astype(F32)), 1.0, 0.0
    ).astype(BF)
    spread[...] = table
    total = jnp.zeros((TOK, 1), F32)
    for b in range(CHIPS):
        x = tokens[:, at(place[b] * BK)]
        xs[:, b * BK : (b + 1) * BK] = x
        x = x.astype(F32)
        total = total + jnp.sum(x * x, axis=-1, keepdims=True)
    r = lax.rsqrt(total * (1.0 / D) + EPSILON)
    root[...] = jnp.broadcast_to(r, (TOK, 128))
    for b in range(CHIPS):
        cols = slice(b * BK, (b + 1) * BK)
        g = gain[:, at(place[b] * BK)]
        gains[:, cols] = g
        h = (xs[:, cols].astype(F32) * r * g).astype(BF)
        hidden[:, cols] = h
        outgoing[:, cols] = tn(table, h).astype(BF)
        outgoing[:, D + b * BK : D + (b + 1) * BK] = tn(
            table, cotangent[:, at(place[b] * BK)]
        ).astype(BF)
    outgoing[:, 2 * D :] = tn(table, half).astype(BF)


def flip_kernel(mine, other, flipped):
    for b in range(16):
        cols = slice(b * BK, (b + 1) * BK)
        flipped[cols, 0:SLOTS] = mine[:, cols].T
        flipped[cols, SLOTS : 2 * SLOTS] = other[:, cols].T


EARLY = (0, 1, 3, 4, 2, 5)
LATE = (7, 6)


def products(rows, pieces, blocks, totals, logits):
    for b, piece in zip(blocks, pieces):
        x = rows[:, b * BK : (b + 1) * BK]
        y = rows[:, D + b * BK : D + (b + 1) * BK]
        totals[0] = totals[0] + nn(x, piece[0:256, :])
        totals[1] = totals[1] + nn(x, piece[256:512, :])
        totals[2] = totals[2] + nn(y, piece[512:768, :])
        for c in range(2):
            logits = logits + nt(x[:, c * TOK : (c + 1) * TOK], router_rows(piece, c))
    return totals, logits


def fetch(sources, held, sems):
    copies = []
    for n, source in enumerate(sources):
        for h, part in enumerate(source):
            target = held.at[n] if len(source) == 1 else held.at[n, :, SIDES[h]]
            copies.append(pltpu.make_async_copy(part, target, sems.at[n, h]))
    for c in copies:
        c.start()
    for c in copies:
        c.wait()
    return [held.at[n] for n in range(len(sources))]


def keep_products(rows, pieces, sums, slot_logits):
    totals, logits = products(
        rows, pieces, EARLY, [jnp.zeros((SLOTS, HALF), F32)] * 3, jnp.zeros((SLOTS, 64), F32)
    )
    for m in range(3):
        sums[:, m * HALF : (m + 1) * HALF] = totals[m]
    slot_logits[...] = logits


def early_kernel(rows, *refs):
    sums, slot_logits, routed, held, sems = refs[7:]
    pieces = fetch([refs[n : n + 1] for n in range(5)] + [refs[5:7]], held, sems)
    keep_products(rows, pieces, sums, slot_logits)
    for n in range(6):
        for c in range(2):
            routed[:, (2 * n + c) * TOK : (2 * n + c + 1) * TOK] = router_rows(pieces[n], c)


def early_other_kernel(rows, held, sums, slot_logits):
    keep_products(rows, [held.at[n] for n in range(6)], sums, slot_logits)


def late_kernel(place, *refs):
    act, scaled, grad_gate, grad_up, routed, held, sems = refs[9:]
    pieces = fetch([refs[6:7], refs[7:9]], held, sems)
    lane = lax.broadcasted_iota(jnp.int32, (SLOTS, 64), 1)
    for i in range(2):
        rows, sums, slot_logits = refs[3 * i : 3 * i + 3]
        out = slice(i * SLOTS, (i + 1) * SLOTS)
        totals, logits = products(
            rows, pieces, LATE, [sums[:, m * HALF : (m + 1) * HALF] for m in range(3)],
            slot_logits[...],
        )
        picked = rows[:, 2 * D : 2 * D + 64].astype(F32) > 0.5
        raised = jnp.where(picked, jnp.exp(logits), 0.0)
        mine = jnp.sum(jnp.where(lane == place[9], raised, 0.0), axis=-1, keepdims=True)
        total = jnp.sum(raised, axis=-1, keepdims=True)
        w = jnp.where(total > 0.0, mine / jnp.where(total > 0.0, total, 1.0), 0.0)
        gate, up, back = totals
        sig = jax.nn.sigmoid(gate)
        silu = gate * sig
        active = silu * up
        back = back * w
        act[out, :] = active.astype(BF)
        scaled[out, :] = (active * w).astype(BF)
        grad_gate[out, :] = (back * up * sig * (1.0 + gate * (1.0 - sig))).astype(BF)
        grad_up[out, :] = (back * silu).astype(BF)
    for n in range(2):
        for c in range(2):
            routed[:, (2 * n + c) * TOK : (2 * n + c + 1) * TOK] = router_rows(pieces[n], c)


def output_kernel(rows, act, grad_gate, grad_up, first, last, *refs):
    i = 1 if len(refs) == 2 else 0
    some = slice(i * SLOTS, (i + 1) * SLOTS)
    copies = []
    if i == 0:
        received, target, gain, out, sems = refs
    else:
        out, gain = refs
    for b in range(CHIPS):
        cols = slice(b * BK, (b + 1) * BK)
        more = slice(D + b * BK, D + (b + 1) * BK)
        piece = first.at[EARLY.index(b)] if b in EARLY else last.at[LATE.index(b)]
        made = nt(act[some, :], piece[512:768, :])
        total = nt(grad_gate[some, :], piece[0:256, :])
        total = total + nt(grad_up[some, :], piece[256:512, :])
        gain[:, cols] = jnp.sum(total * rows[:, cols].astype(F32), axis=0, keepdims=True)
        if i == 0:
            made = made + received[:, cols].astype(F32)
            total = total + received[:, more].astype(F32)
        out[:, cols] = made.astype(BF)
        out[:, more] = total.astype(BF)
        if i == 0 and b % 2:
            for h, start in enumerate((0, D)):
                span = slice(start + (b - 1) * BK, start + (b + 1) * BK)
                copies.append(
                    pltpu.make_async_copy(out.at[:, span], target.at[:, span], sems.at[b // 2, h])
                )
                copies[-1].start()
    for c in copies:
        c.wait()


HALVED = (3, 5)


def grads_kernel(blocks):
    def kernel(flipped, scaled, grad_gate, grad_up, *refs):
        outs, stage, sems = refs[:-2], refs[-2], refs[-1]
        copies = {}
        for n, b in enumerate(blocks):
            slot = n % 3
            if n >= 3:
                for c in copies[n - 3]:
                    c.wait()
            x = flipped[b * BK : (b + 1) * BK, :]
            stage[slot, 0:256, :] = nn(x, grad_gate[...]).astype(BF)
            stage[slot, 256:512, :] = nn(x, grad_up[...]).astype(BF)
            stage[slot, 512:768, :] = nn(
                flipped[D + b * BK : D + (b + 1) * BK, :], scaled[...]
            ).astype(BF)
            if b in HALVED:
                copies[n] = [
                    pltpu.make_async_copy(stage.at[slot, :, side], out, sems.at[slot, h])
                    for h, (side, out) in enumerate(zip(SIDES, (outs[n], outs[-1])))
                ]
            else:
                copies[n] = [pltpu.make_async_copy(stage.at[slot], outs[n], sems.at[slot, 0])]
            for c in copies[n]:
                c.start()
        for n in range(max(0, len(blocks) - 3), len(blocks)):
            for c in copies[n]:
                c.wait()

    return kernel


def block_of(routed_early, routed_late, b):
    source, n = (routed_early, EARLY.index(b)) if b in EARLY else (routed_late, LATE.index(b))
    return source[:, n * BK : (n + 1) * BK]


def pick_weights(hidden, routed_early, routed_late, chosen):
    logits = jnp.zeros((TOK, 64), F32)
    for b in range(CHIPS):
        r = block_of(routed_early, routed_late, b)
        logits = logits + nt(hidden[:, b * BK : (b + 1) * BK], r)
    raised = jnp.where(chosen[:, :64] > 0.5, jnp.exp(logits), 0.0)
    return raised / jnp.sum(raised, axis=-1, keepdims=True)


def mix_kernel(place, returned, cotangent, spread, chosen, hidden, routed_early, routed_late, gains, gain_mine, gain_other, weight, grad_logits, parts, work):
    w = pick_weights(hidden, routed_early, routed_late, chosen)
    weight[...] = w
    per_slot = jnp.zeros((SLOTS, 1), F32)
    for b in range(CHIPS):
        c = tn(spread[...], cotangent[:, at(place[b] * BK)])
        y = returned[:, b * BK : (b + 1) * BK].astype(F32)
        per_slot = per_slot + jnp.sum(c * y, axis=-1, keepdims=True)
    slot = lax.broadcasted_iota(jnp.int32, (SLOTS, 64), 0)
    who = lax.broadcasted_iota(jnp.int32, (SLOTS, 64), 1)
    spots = jnp.where(who == slot // CAP, per_slot, 0.0)
    high = spots.astype(BF)
    rest = spots - high.astype(F32)
    middle = rest.astype(BF)
    low = (rest - middle.astype(F32)).astype(BF)
    table = spread[...]
    grad_weights = nn(table, high) + nn(table, middle) + nn(table, low)
    inner = jnp.sum(w * grad_weights, axis=-1, keepdims=True)
    g = w * (grad_weights - inner)
    grad_logits[...] = g
    gh, gl = split(g)
    for b in range(CHIPS):
        cols = slice(b * BK, (b + 1) * BK)
        h = hidden[:, cols]
        part = tn(gh, h) + tn(gl, h)
        gain = gain_mine[:, cols] + gain_other[:, cols] + jnp.sum(
            part * block_of(routed_early, routed_late, b).astype(F32), axis=0, keepdims=True
        )
        gain_high, gain_low = split(gain / gains[:, cols])
        for c in range(2):
            home = place[b] * 2 + c
            lanes = slice(c * TOK, (c + 1) * TOK)
            parts[home, 0:64, :] = part[:, lanes].astype(BF)
            work[pl.ds(home, 1), :] = gain_high[:, lanes].astype(F32)
            work[pl.ds(16 + home, 1), :] = gain_low[:, lanes].astype(F32)
    whole = work[...].astype(BF)
    for d in range(16):
        parts[d, 64:96, :] = whole


def norm_kernel(place, returned, spread, weight, grad_logits, routed_early, routed_late, xs, gains, root, mixed, d_tokens, work):
    who = lax.broadcasted_iota(jnp.int32, (64, SLOTS), 0)
    slot = lax.broadcasted_iota(jnp.int32, (64, SLOTS), 1)
    widen = (who == slot // CAP).astype(F32).astype(BF)
    high, low = split(weight[...])
    table = spread[...]
    mask = table.astype(F32)
    blend_high = (nn(high, widen) * mask).astype(BF)
    blend_low = (nn(low, widen) * mask).astype(BF)
    gh, gl = split(grad_logits[...])
    r = root[:, 0:1]
    inner = jnp.zeros((TOK, 1), F32)
    for b in range(CHIPS):
        cols = slice(b * BK, (b + 1) * BK)
        y = returned[:, cols]
        mixed[:, at(place[b] * BK)] = (nn(blend_high, y) + nn(blend_low, y)).astype(BF)
        rt = block_of(routed_early, routed_late, b)
        grad = nn(table, returned[:, D + b * BK : D + (b + 1) * BK]) + nn(gh, rt) + nn(gl, rt)
        scaled = grad * gains[:, cols]
        work[:, cols] = scaled
        inner = inner + jnp.sum(scaled * xs[:, cols].astype(F32), axis=-1, keepdims=True)
    factor = inner * (r * r * r) * (1.0 / D)
    for b in range(CHIPS):
        cols = slice(b * BK, (b + 1) * BK)
        d_tokens[:, at(place[b] * BK)] = (
            work[:, cols] * r - xs[:, cols].astype(F32) * factor
        ).astype(BF)


def total_kernel(place, here, *refs):
    halves, give, keep = refs[:6], refs[6], refs[7]
    core = place[8]
    for m in range(3):
        for out, side in ((give, 1 - core), (keep, core)):
            rows = at(m * BK + side * TOK, TOK)
            for h, cols in enumerate(SIDES):
                total = here[rows, cols].astype(F32)
                for v in halves[h::2]:
                    total = total + v[rows, :].astype(F32)
                out[m * TOK : (m + 1) * TOK, cols] = total.astype(BF)


def share_kernel(parts, shares):
    total = parts[0].astype(F32)
    for d in range(1, 16):
        total = total + parts[d].astype(F32)
    for e in range(WIN):
        shares[e, 0:64, :] = total[0:64]
        shares[e, 64:80, :] = total[64:80] + total[80:96]


def small_kernel(shares, d_router, d_gain):
    total = shares[0]
    for e in range(1, WIN):
        total = total + shares[e]
    d_router[...] = total[0:64]
    d_gain[...] = total[64:80]


def finish_kernel(place, keep, other, *outs):
    core = place[8]
    for m, out in enumerate(outs):
        rows = slice(m * TOK, (m + 1) * TOK)
        out[:, at(core * HALF, HALF)] = keep[rows, :]
        out[:, at((1 - core) * HALF, HALF)] = other[rows, :]


def perm(move):
    pairs = []
    for x in range(2):
        for z in range(4):
            for c in range(2):
                tx, tz, tc = move(x, z, c)
                pairs.append(((x * 4 + z) * 2 + c, (tx * 4 + tz % 4) * 2 + tc))
    return pairs


SIBLING = perm(lambda x, z, c: (x, z, 1 - c))
ACROSS = perm(lambda x, z, c: (1 - x, z, c))
AHEAD = perm(lambda x, z, c: (x, z + 1, c))
BEHIND = perm(lambda x, z, c: (x, z + 3, c))


DP = ("chip", "core")


def send(v, pairs):
    return lax.ppermute(v, DP, pairs)


def gather_pieces(own):
    across = send(own, ACROSS)
    own_3 = send(own, AHEAD)
    own_1 = send(own, BEHIND)
    own_2 = send(own_3, AHEAD)
    across_1 = [send(across[:, side], BEHIND) for side in SIDES]
    across_3 = send(across, AHEAD)
    across_2 = [send(v, BEHIND) for v in across_1]
    return ([own], [own_1], [own_2], [own_3], [across], across_1, across_2, [across_3])


def plus(*values):
    total = values[0].astype(F32)
    for v in values[1:]:
        total = total + v.astype(F32)
    return total.astype(BF)


def reduce_pieces(parts):
    across_2 = send(parts[6], BEHIND)
    across_1 = [send(v, AHEAD) for v in (parts[5], parts[9])]
    own_2 = send(parts[2], AHEAD)
    across_3 = [send(plus(parts[7][:, side], across_2[:, side]), BEHIND) for side in SIDES]
    own_3 = [send(v, BEHIND) for v in (parts[3], parts[8])]
    own_1 = [send(plus(parts[1][:, side], own_2[:, side]), AHEAD) for side in SIDES]
    base, ahead = lax.optimization_barrier((parts[4], across_1[1]))
    across = [
        send(v, ACROSS)
        for v in (
            plus(parts[4][:, LEFT], across_1[0], across_3[0]),
            plus(base[:, RIGHT], ahead, across_3[1]),
        )
    ]
    return parts[0], *own_1, *own_3, *across


def exchange(v, axis):
    return lax.all_to_all(v, axis, split_axis=0, concat_axis=0, tiled=True)


def body(
    tokens, norm_gain, router_weight, expert_ids, gate_weight, up_weight, down_weight, cotangent
):
    chip = lax.axis_index("chip")
    core = lax.axis_index("core")
    x, z = chip >> 2, chip & 3
    rel = jnp.arange(16, dtype=jnp.int32)
    chips = ((x ^ ((rel >> 2) & 1)) * 4 + ((z + rel) & 3)).astype(jnp.int32)
    mine = jnp.where(rel == 8, core, lax.axis_index("expert")).astype(jnp.int32)
    place = jnp.where(rel < 8, chips, mine)

    weights = (gate_weight[0], up_weight[0], down_weight[0])
    away, keep_own = call(
        pack_kernel, [sds((400, HALF), BF)] * 2, place, *weights, router_weight.T, smem=1,
        limit=MiB(2), far=(1, 2, 3), dram=(4,), scratch=[pltpu.SemaphoreType.DMA((2, 3))],
    )
    other = send(away, SIBLING)
    hidden, xs, gains, root, spread, chosen, sent = call(
        dispatch_kernel,
        [pltpu.HBM((TOK, D), BF), pltpu.HBM((TOK, D), BF), pltpu.HBM((1, D), F32),
         pltpu.HBM((TOK, 128), F32), pltpu.HBM((TOK, SLOTS), BF), pltpu.HBM((TOK, 128), F32),
         pltpu.HBM((SLOTS, WIDE), BF)],
        place, tokens, cotangent, norm_gain[None], expert_ids, smem=1, dram=(1, 2, 3),
        limit=MiB(12),
    )
    own = call(join_kernel, sds((ROWS, HALF), BF), place, keep_own, other, smem=1, limit=MiB(3))
    pieces = gather_pieces(own)

    rows = exchange(sent.reshape(WIN, CAP, WIDE), "expert").reshape(SLOTS, WIDE)
    rows_other = send(rows, SIBLING)
    flipped = call(flip_kernel, sds((2 * D, 2 * SLOTS), BF), rows, rows_other, limit=MiB(12))
    shapes = [sds((SLOTS, 3 * HALF), F32), sds((SLOTS, 64), F32)]
    sums, slot_logits, routed_early, held_early = call(
        early_kernel,
        shapes + [pltpu.HBM((64, 6 * BK), BF), pltpu.VMEM((6, ROWS, HALF), BF)],
        rows, *[v for b in EARLY for v in pieces[b]], limit=MiB(6), far=range(1, 8),
        scratch=[pltpu.SemaphoreType.DMA((6, 2))],
    )
    sums_other, logits_other = call(
        early_other_kernel, shapes, rows_other, held_early, limit=MiB(6),
    )
    act, scaled, grad_gate, grad_up, routed_late, held_late = call(
        late_kernel,
        [sds((2 * SLOTS, HALF), BF)] * 4
        + [pltpu.HBM((64, 2 * BK), BF), pltpu.VMEM((2, ROWS, HALF), BF)],
        place, rows, sums, slot_logits, rows_other, sums_other, logits_other,
        *[v for b in LATE for v in pieces[b]], smem=1, limit=MiB(8), far=(7, 8, 9),
        scratch=[pltpu.SemaphoreType.DMA((2, 2))],
    )
    shapes = [sds((SLOTS, 2 * D), BF), sds((1, D), F32)]
    operands = (act, grad_gate, grad_up, held_early, held_late)
    partial, gain_other = call(output_kernel, shapes, rows_other, *operands, limit=MiB(6))
    received = send(partial, SIBLING)
    output, gain_mine = call(
        output_kernel, [pltpu.HBM((SLOTS, 2 * D), BF), sds((1, D), F32)],
        rows, *operands, received, limit=MiB(8), out_specs=[HBM, VMEM],
        scratch=[pltpu.VMEM((SLOTS, 2 * D), BF), pltpu.SemaphoreType.DMA((4, 2))],
    )
    returned = exchange(output.reshape(WIN, CAP, 2 * D), "expert")
    returned = returned.reshape(SLOTS, 2 * D)
    parts = {}
    for blocks, extra in (((6, 5, 2), 9), ((3, 7, 1, 4, 0), 8)):
        shapes = [pltpu.HBM((768, BK if b in HALVED else HALF), BF) for b in blocks]
        shapes.append(pltpu.HBM((768, BK), BF))
        made = call(
            grads_kernel(blocks), shapes, flipped, scaled, grad_gate, grad_up,
            limit=MiB(5), far_out=True,
            scratch=[pltpu.VMEM((3, 768, HALF), BF), pltpu.SemaphoreType.DMA((3, 2))],
        )
        parts.update(zip(blocks + (extra,), made))
    give, keep = call(
        total_kernel, [sds((384, HALF), BF)] * 2, place, *reduce_pieces(parts),
        smem=1, limit=MiB(6),
    )
    fetched = send(give, SIBLING)
    d_weights = call(
        finish_kernel, [pltpu.HBM((TOK, FF), BF)] * 3, place, keep, fetched,
        smem=1, limit=MiB(4),
    )

    weight, grad_logits, shares = call(
        mix_kernel,
        [sds((TOK, 64), F32), sds((TOK, 64), F32), pltpu.HBM((16, 96, TOK), BF)],
        place, returned, cotangent, spread, chosen, hidden, routed_early, routed_late, gains,
        gain_mine, gain_other, smem=1, dram=range(2, 9), limit=MiB(12),
        scratch=[pltpu.VMEM((32, TOK), F32)],
    )
    shares = exchange(shares, DP)
    shares = call(share_kernel, sds((8, 80, TOK), F32), shares, limit=MiB(2))
    shares = exchange(shares, "expert")
    d_router, d_gain = call(
        small_kernel, [pltpu.HBM((64, TOK), F32), pltpu.HBM((16, TOK), F32)], shares, limit=MiB(2)
    )

    mixed, d_tokens = call(
        norm_kernel, [pltpu.HBM((TOK, D), BF)] * 2,
        place, returned, spread, weight, grad_logits, routed_early, routed_late, xs, gains, root,
        smem=1, dram=(2, 5, 6, 7, 8, 9), limit=MiB(10), scratch=[pltpu.VMEM((TOK, D), F32)],
    )
    return (mixed, d_tokens, d_gain.reshape(D), d_router.T, *[d[None] for d in d_weights])


def MiB(n):
    return n << 20


def solution(mesh):
    grid = Mesh(mesh.devices.reshape(8, 2, 8), ("chip", "core", "expert"))
    every = P(("chip", "core", "expert"), None)
    rows = P("expert", DP, None)
    in_specs = (every, P(), P(DP, None), every, rows, rows, rows, every)
    out_specs = (every, every, P(), P(DP, None), rows, rows, rows)
    return jax.shard_map(body, mesh=grid, in_specs=in_specs, out_specs=out_specs, check_vma=False)
```
